128 devices in a mesh: ep: 16 (over y, z), tp: 8 (over x, core).
Axes of the slice: x: 4, y: 4, z: 4, core: 2. Of those that a mesh axis runs over, the one named last changes fastest.
Arguments:
- tokens: bfloat16 [2048, 4096], P(('ep', 'tp')), may hold values from -6 to 6
- routes: int32 [2048, 2], P(('ep', 'tp')), may hold values from 0 to 15, all different within a row; in each aligned block of 16 rows (0 to 15, 16 to 31, ...) at most 4 rows name the same one
- combine: float32 [2048, 2], P(('ep', 'tp')), may hold values from 0.25 to 1
- gate_weight: bfloat16 [16, 4096, 4096], P('ep', None, 'tp'), may hold values from -0.09375 to 0.09375
- up_weight: bfloat16 [16, 4096, 4096], P('ep', None, 'tp'), may hold values from -0.09375 to 0.09375
- down_weight: bfloat16 [16, 4096, 4096], P('ep', 'tp'), may hold values from -0.09375 to 0.09375
Outputs:
- moe_output: bfloat16 [2048, 4096], P(('ep', 'tp'))
The draws below stay inside these ranges and needn't reach their ends.
Inputs may be any that keep to these rules, and one draw needn't show every extreme that they name: `routes`: each row names 2 different experts. Among the rows of one device no expert is named more than 4 times, and in every draw some expert is named exactly 4 times by the rows of some device.
All inputs are finite; a program needn't handle non-finite values.
Results may differ from the reference program's by a relative error of at most 0.015.
Values may be sent and summed in bfloat16 or wider, within the bound.
A program may use at most 64 MiB of HBM per device.

```python
import math
import jax
import jax.numpy as jnp
import numpy as np
from jax import lax

D = 4096
FF = 4096
TOP = 2
TOK_DEV = 16
E = 16
FF_DEV = 512
C = 4
TOKENS = 2048
N_TP = 8
DEVICES = 128


def block_scale(rng, dims, split, smallest, top_value):
    def one(dim, parts):
        steps = jax.random.uniform(jax.random.fold_in(jax.random.fold_in(rng, 6), dim), (parts,), jnp.float32, smallest / len(split), top_value / len(split))
        return jnp.repeat(jnp.exp(steps), dims[dim] // parts).reshape((-1,) + (1,) * (len(dims) - dim - 1))

    gain = one(*split[0])
    for cut in split[1:]:
        gain = gain * one(*cut)
    return gain


def assign_block(stream_key, own, number, rows, number_of, top, bound, slope):
    ranking = jax.random.permutation(stream_key, number_of)
    crowded, common = shares(number_of, rows * top, bound, slope, True), shares(number_of, rows * top, bound, slope, False)
    places = jnp.arange(number_of)

    def named(sizes, offset_by):
        used = int((sizes > 0).sum())
        fixed = max(1, used // 4)
        shifted = fixed + (places - fixed + offset_by * (used - fixed)) % max(1, number_of - fixed)
        return jnp.zeros((number_of,), jnp.int32).at[ranking[jnp.where(places < fixed, places, shifted)]].set(jnp.asarray(sizes, jnp.int32))

    sizes = jnp.where(number % 4 == 0, named(crowded, number // 4), named(common, number - number // 4 - 1))
    mixed = jax.random.permutation(jax.random.fold_in(own, 3), number_of)
    giver, sink = mixed[0:number_of // 2 * 2:2], mixed[1:number_of // 2 * 2:2]
    slack = jnp.minimum(sizes[giver] - 1, bound - sizes[sink]) // 2
    slack = jnp.where((giver == ranking[0]) | (sink == ranking[0]) | (sizes[sink] == 0), 0, jnp.maximum(slack, 0))
    shifted = jax.random.randint(jax.random.fold_in(own, 4), (number_of // 2,), 0, 1 << 20) % (slack + 1)
    sizes = sizes.at[giver].add(-shifted).at[sink].add(shifted)
    items = jnp.searchsorted(jnp.cumsum(sizes), jnp.arange(rows * top), side="right").astype(jnp.int32)
    table = items.reshape(top, rows).T
    table = table[jax.random.permutation(jax.random.fold_in(own, 1), rows)]
    offset_by = jax.random.randint(jax.random.fold_in(own, 2), (rows, 1), 0, top)
    return jnp.take_along_axis(table, (jnp.arange(top)[None, :] + offset_by) % top, axis=1)


def shares(number_of, total, bound, skew, full):
    loads = [(1 << 20) // math.isqrt(grade ** skew) + 1 for grade in range(1, number_of + 1)]
    largest = bound if full else min(bound, max(-(-total // number_of), total * loads[0] // sum(loads)))
    least = 1 if total - largest >= number_of - 1 else 0
    holding, surplus = [largest] + [least] * (number_of - 1), total - largest - least * (number_of - 1)
    while surplus > 0:
        candidates = [i for i in range(1, number_of) if holding[i] < largest] or [i for i in range(1, number_of) if holding[i] < bound]
        pool, remaining = sum([loads[i] for i in candidates]), surplus
        for i in candidates:
            addition = min(bound - holding[i], max(1, remaining * loads[i] // pool), surplus)
            holding[i] = holding[i] + addition
            surplus = surplus - addition
    return np.array(holding)


def centred(stream_key, shape, width, bound, split=(), kind=jnp.bfloat16):
    drawn = jax.random.normal(stream_key, shape, jnp.float32) * width
    if len(split) > 0:
        drawn = block_scale(stream_key, shape, split, -0.22, 0.18) * drawn
    return jnp.clip(drawn, min=-bound, max=bound).astype(kind)


def setup_inputs(seed: int = 0) -> dict:
    splits = jax.random.split(jax.random.key(seed), 7)
    tokens = centred(splits[0], (TOKENS, D), 1.0, 6.0, ((0, 128),))
    routes_keys = jax.random.split(jax.random.fold_in(splits[1], 1), TOKENS // TOK_DEV)
    routes_turns = jax.random.permutation(jax.random.fold_in(splits[1], 3), TOKENS // TOK_DEV)
    routes = jax.vmap(lambda own, number: assign_block(jax.random.fold_in(splits[1], 2), own, number, TOK_DEV, E, TOP, C, 2))(routes_keys, routes_turns).reshape((TOKENS, TOP))
    combine = jnp.clip(0.25 + 0.75 * jax.random.uniform(splits[2], (TOKENS, TOP), jnp.float32) ** block_scale(splits[2], (TOKENS, TOP), ((0, 128),), -0.2, 0.2), 0.25, 1.0)
    gate_weight = centred(splits[3], (E, D, FF), D ** -0.5, 0.09375, ((0, 16), (2, 8)))
    up_weight = centred(splits[4], (E, D, FF), D ** -0.5, 0.09375, ((0, 16), (2, 8)))
    down_weight = centred(splits[5], (E, FF, D), FF ** -0.5, 0.09375, ((0, 16), (1, 8)))
    return dict(tokens=tokens, routes=routes, combine=combine, gate_weight=gate_weight, up_weight=up_weight, down_weight=down_weight)


def reference(tokens, routes, combine, gate_weight, up_weight, down_weight):
    assignments = TOK_DEV * TOP
    flat_ids = routes.reshape(DEVICES, assignments).astype(jnp.int32)
    onehot = (flat_ids[:, :, None] == jnp.arange(E, dtype=jnp.int32)[None, None, :]).astype(jnp.int32)
    earlier = jnp.cumsum(onehot, axis=1) - onehot
    slot_index = jnp.sum(earlier * onehot, axis=2)
    target = flat_ids * C + slot_index
    selector = (target[:, :, None] == jnp.arange(E * C, dtype=jnp.int32)[None, None, :]).astype(jnp.float32)
    repeated = jnp.repeat(tokens.reshape(DEVICES, TOK_DEV, D), TOP, axis=1).astype(jnp.float32)
    buffer = jnp.einsum("sak,sad->skd", selector, repeated, precision=lax.Precision.HIGHEST).astype(jnp.bfloat16)
    buffer = buffer.reshape(DEVICES, E, C, D).transpose(1, 0, 2, 3).reshape(E, DEVICES * C, D)

    def expert(operands):
        inputs, w_gate, w_up, w_down = operands
        gate_values = jnp.dot(inputs, w_gate, preferred_element_type=jnp.float32)
        up_values = jnp.dot(inputs, w_up, preferred_element_type=jnp.float32)
        hidden = (jax.nn.silu(gate_values) * up_values).astype(jnp.bfloat16)
        hidden_split = hidden.reshape(DEVICES * C, N_TP, FF_DEV).astype(jnp.float32)
        down_split = w_down.reshape(N_TP, FF_DEV, D).astype(jnp.float32)
        group_parts = jnp.einsum("rgf,gfd->grd", hidden_split, down_split, precision=lax.Precision.HIGHEST).astype(jnp.bfloat16)
        return jnp.sum(group_parts.astype(jnp.float32), axis=0).astype(jnp.bfloat16)

    expert_results = lax.map(expert, (buffer, gate_weight, up_weight, down_weight))
    returned = expert_results.reshape(E, DEVICES, C, D).transpose(1, 0, 2, 3).reshape(DEVICES, E * C, D).astype(jnp.float32)
    picked = jnp.einsum("sak,skd->sad", selector, returned, precision=lax.Precision.HIGHEST).reshape(TOKENS, TOP, D)
    return jnp.sum(combine[:, :, None] * picked, axis=1).astype(jnp.bfloat16)
```

```python
import jax
import jax.numpy as jnp
from jax import lax
from jax.experimental import pallas as pl
from jax.experimental.pallas import tpu as pltpu
from jax.sharding import PartitionSpec as P

MESH = pl.DeviceIdType.MESH
F32 = jnp.float32
BF16 = jnp.bfloat16
CW = 512
NY = 4
NZ = 4
NX = 4
IN_ORDER = (0, 1, 3, 2)
OUT_ORDER = (2, 1, 3, 0)
Z_ORDER = (2, 1, 3, 0)


def kernel(
    tok_ref, info_ref, wg_hbm, wu_hbm, wd_hbm, out_ref,
    tr, infos, pk, xs, wg, wu, wd, accg, accu, hid, sel, whi, wlo,
    ds, dr, q, sa, ra, sb, rb, s1p, r1m, s1m, r1p, fin, ret, osl, outr,
    w_sem, t_send, t_recv, i_send, i_recv, a_send, a_recv,
    g_send, g_recv, d_send, d_recv, r_send, r_recv, b_send, b_recv, o_send, o_recv,
):
    ep = lax.axis_index("ep")
    tp = lax.axis_index("tp")
    y, z = ep // NZ, ep % NZ
    x, c = tp // 2, tp % 2

    def on_tp(other):
        return {"ep": ep, "tp": other}

    def on_ep(other):
        return {"ep": other, "tp": tp}

    def remote(src, dst, send_sem, recv_sem, device):
        copy = pltpu.make_async_remote_copy(
            src_ref=src, dst_ref=dst, send_sem=send_sem, recv_sem=recv_sem,
            device_id=device, device_id_type=MESH,
        )
        copy.start()
        return copy

    loads = []
    for n, (src, dst) in enumerate(((wg_hbm, wg), (wu_hbm, wu), (wd_hbm, wd))):
        load = pltpu.make_async_copy(src, dst, w_sem.at[n])
        load.start()
        loads.append(load)

    barrier = pltpu.get_barrier_semaphore()
    for j in range(1, 8):
        pl.semaphore_signal(barrier, inc=1, device_id=on_tp((tp + j) % 8), device_id_type=MESH)
    for dy in range(NY):
        for dz in range(NZ):
            if dy or dz:
                other = ((y + dy) % NY) * NZ + (z + dz) % NZ
                pl.semaphore_signal(barrier, inc=1, device_id=on_ep(other), device_id_type=MESH)
    pl.semaphore_wait(barrier, 22)

    sent = []
    first = []
    for j in range(1, 8):
        other = (tp + j) % 8
        first.append(remote(info_ref, infos.at[tp], i_send.at[j], i_recv.at[j], on_tp(other)))
    for j in range(1, 8):
        other = (tp + j) % 8
        cols = pl.ds(pl.multiple_of(other * CW, CW), CW)
        first.append(remote(tok_ref.at[:, cols], tr.at[tp], t_send.at[j], t_recv.at[j], on_tp(other)))
    infos[tp] = info_ref[...]
    tr[tp] = tok_ref[:, pl.ds(pl.multiple_of(tp * CW, CW), CW)]
    for copy in first[:7]:
        copy.wait_recv()
    sent += first

    lane8 = lax.broadcasted_iota(jnp.int32, (8, 128), 1) // 16
    info = jnp.zeros((8, 128), F32)
    for b in range(8):
        info = info + jnp.where(lane8 == b, infos[b], 0.0)
    row = lax.broadcasted_iota(jnp.int32, (512, 128), 0)
    lane = lax.broadcasted_iota(jnp.int32, (512, 128), 1)
    expert = (row // 32).astype(F32)
    slot = (row % 4).astype(F32)
    same = (lane // 16) == ((row % 32) // 4)
    first_of = jnp.where(info[0:1] == expert, 1.0, 0.0)
    second_of = jnp.where(info[1:2] == expert, 1.0, 0.0)
    named = first_of + second_of
    urow = lax.broadcasted_iota(jnp.int32, (128, 128), 0)
    ulane = lax.broadcasted_iota(jnp.int32, (128, 128), 1)
    before = jnp.where((urow < ulane) & ((urow // 16) == (ulane // 16)), 1.0, 0.0).astype(BF16)
    count = jnp.dot(named.astype(BF16), before, preferred_element_type=F32)
    hit = same & (count == slot)
    sel[...] = jnp.where(hit, named, 0.0).astype(BF16)
    weight = jnp.where(hit, first_of * info[2:3] + second_of * info[3:4], 0.0)
    weight = weight.T
    high = weight.astype(BF16)
    whi[...] = high
    wlo[...] = (weight - high.astype(F32)).astype(BF16)

    for copy in first[7:]:
        copy.wait_recv()
    picked = jnp.dot(sel[...], tr[...].reshape(128, CW), preferred_element_type=F32)
    pk[...] = picked.astype(BF16).reshape(16, 32, CW)
    xs[tp, ep] = pk[ep]

    spread = {}
    for dy in IN_ORDER:
        for dz in Z_ORDER:
            if dy or dz:
                other = ((y + dy) % NY) * NZ + (z + dz) % NZ
                k = dy * NZ + dz
                spread[dy, dz] = remote(
                    pk.at[other], xs.at[tp, ep], a_send.at[k], a_recv.at[k], on_ep(other)
                )
    sent += list(spread.values())

    mate = x * 2 + (1 - c)
    right = ((x + 1) % NX) * 2 + c
    left = ((x + 3) % NX) * 2 + c
    far = ((x + 2) % NX) * 2 + c

    to_mate, to_right, to_left = [], [], []
    for i, dy in enumerate(IN_ORDER):
        for dz in range(NZ):
            if dy or dz:
                spread[dy, dz].wait_recv()
        ys = ((y + NY - dy) % NY) * NZ
        block = xs.at[tp, pl.ds(ys, 4)]
        to_right.append(remote(block, block, g_send.at[0, i], g_recv.at[0, i], on_tp(right)))
        to_left.append(remote(block, block, g_send.at[1, i], g_recv.at[1, i], on_tp(left)))
        to_mate.append(remote(block, block, g_send.at[2, i], g_recv.at[2, i], on_tp(mate)))
    sent += to_right + to_left + to_mate
    loads[0].wait()
    loads[1].wait()
    for copy in to_mate:
        copy.wait_recv()

    def gate_up(chip, fresh):
        gate = up = None
        for core in range(2):
            t = chip * 2 + core
            a = xs[t].reshape(512, CW)
            rows = pl.ds(pl.multiple_of(t * CW, CW), CW)
            g1 = jnp.dot(a, wg[rows, :], preferred_element_type=F32)
            u1 = jnp.dot(a, wu[rows, :], preferred_element_type=F32)
            gate = g1 if gate is None else gate + g1
            up = u1 if up is None else up + u1
        if fresh:
            accg[...] = gate
            accu[...] = up
        else:
            accg[...] += gate
            accu[...] += up

    gate_up(x, True)

    on_right, on_left, mate_left, mate_right = [], [], [], []
    for i, dy in enumerate(IN_ORDER):
        ys = ((y + NY - dy) % NY) * NZ
        to_right[i].wait_recv()
        half = xs.at[left, pl.ds(ys, 2)]
        on_right.append(remote(half, half, g_send.at[3, i], g_recv.at[3, i], on_tp(right)))
        block = xs.at[left, pl.ds(ys, 4)]
        mate_left.append(remote(block, block, g_send.at[5, i], g_recv.at[5, i], on_tp(mate)))
        to_left[i].wait_recv()
        half = xs.at[right, pl.ds(ys + 2, 2)]
        on_left.append(remote(half, half, g_send.at[4, i], g_recv.at[4, i], on_tp(left)))
        block = xs.at[right, pl.ds(ys, 4)]
        mate_right.append(remote(block, block, g_send.at[6, i], g_recv.at[6, i], on_tp(mate)))
    sent += on_right + on_left + mate_left + mate_right
    for copy in mate_left:
        copy.wait_recv()
    gate_up((x + 3) % NX, False)
    mate_far = []

    def pass_far(i):
        ys = ((y + NY - IN_ORDER[i]) % NY) * NZ
        on_right[i].wait_recv()
        half = xs.at[far, pl.ds(ys, 2)]
        mate_far.append(remote(half, half, g_send.at[7, i], g_recv.at[7, i], on_tp(mate)))
        on_left[i].wait_recv()
        half = xs.at[far, pl.ds(ys + 2, 2)]
        mate_far.append(remote(half, half, g_send.at[8, i], g_recv.at[8, i], on_tp(mate)))

    pass_far(0)
    pass_far(1)
    for copy in mate_right:
        copy.wait_recv()
    gate_up((x + 1) % NX, False)
    pass_far(2)
    pass_far(3)
    sent += mate_far
    for copy in mate_far:
        copy.wait_recv()
    gate_up((x + 2) % NX, False)

    gate = accg[...]
    hid[...] = (gate / (1.0 + jnp.exp(-gate)) * accu[...]).astype(BF16)
    loads[2].wait()

    pair = {}

    def down(k):
        chip = (x + k) % NX
        for own in (False, True):
            t = chip * 2 + (c if own else 1 - c)
            cols = pl.ds(pl.multiple_of(t * CW, CW), CW)
            part = jnp.dot(hid[...], wd[:, cols], preferred_element_type=F32)
            part = part.astype(BF16).reshape(16, 32, CW)
            if own:
                q[k] = part
            else:
                ds[k] = part
                pair[k] = remote(ds.at[k], dr.at[k], d_send.at[k], d_recv.at[k], on_tp(mate))

    def chip_sum(k, start, size):
        rows = pl.ds(start, size)
        return q[k, rows].astype(F32) + dr[k, rows].astype(F32)

    down(2)
    down(1)
    pair[2].wait_recv()
    far_right, far_left = [], []
    for i, dy in enumerate(OUT_ORDER):
        yd = ((y + dy) % NY) * NZ
        sa[i] = chip_sum(2, yd, 2).astype(BF16)
        far_right.append(remote(sa.at[i], ra.at[i], r_send.at[0, i], r_recv.at[0, i], on_tp(right)))
        sb[i] = chip_sum(2, yd + 2, 2).astype(BF16)
        far_left.append(remote(sb.at[i], rb.at[i], r_send.at[1, i], r_recv.at[1, i], on_tp(left)))
    down(3)
    down(0)
    sent += list(pair.values()) + far_right + far_left
    pair[1].wait_recv()
    pair[3].wait_recv()
    near = [[], [], [], []]
    for i, dy in enumerate(OUT_ORDER):
        yd = ((y + dy) % NY) * NZ
        s1p[i, 1] = chip_sum(1, yd + 2, 2).astype(BF16)
        near[0].append(remote(s1p.at[i, 1], r1m.at[i, 1], r_send.at[2, i], r_recv.at[2, i], on_tp(right)))
        s1m[i, 0] = chip_sum(3, yd, 2).astype(BF16)
        near[1].append(remote(s1m.at[i, 0], r1p.at[i, 0], r_send.at[3, i], r_recv.at[3, i], on_tp(left)))
        far_right[i].wait_recv()
        s1p[i, 0] = (chip_sum(1, yd, 2) + ra[i].astype(F32)).astype(BF16)
        near[2].append(remote(s1p.at[i, 0], r1m.at[i, 0], r_send.at[4, i], r_recv.at[4, i], on_tp(right)))
        far_left[i].wait_recv()
        s1m[i, 1] = (chip_sum(3, yd + 2, 2) + rb[i].astype(F32)).astype(BF16)
        near[3].append(remote(s1m.at[i, 1], r1p.at[i, 1], r_send.at[5, i], r_recv.at[5, i], on_tp(left)))
    for copies in near:
        sent += copies
    pair[0].wait_recv()
    back = []
    for i, dy in enumerate(OUT_ORDER):
        yd = ((y + dy) % NY) * NZ
        for copies in near:
            copies[i].wait_recv()
        total = chip_sum(0, yd, 4)
        total = total + r1m[i].astype(F32).reshape(4, 32, CW)
        total = total + r1p[i].astype(F32).reshape(4, 32, CW)
        fin[pl.ds(yd, 4)] = total.astype(BF16)
        for dz in Z_ORDER:
            other = yd + (z + dz) % NZ
            if dy or dz:
                k = dy * NZ + dz
                back.append(remote(fin.at[other], ret.at[ep], b_send.at[k], b_recv.at[k], on_ep(other)))
    ret[ep] = fin[ep]
    sent += back
    for copy in back:
        copy.wait_recv()
    rows = ret[...].reshape(512, CW)
    result = jnp.dot(whi[...], rows, preferred_element_type=F32)
    result = result + jnp.dot(wlo[...], rows, preferred_element_type=F32)
    osl[...] = result.astype(BF16).reshape(8, 16, CW)
    outs = []
    for j in range(1, 8):
        other = (tp + j) % 8
        outs.append(remote(osl.at[other], outr.at[tp], o_send.at[j], o_recv.at[j], on_tp(other)))
    outr[tp] = osl[tp]
    sent += outs
    for copy in outs:
        copy.wait_recv()
    for t in range(8):
        out_ref[:, t * CW:(t + 1) * CW] = outr[t]
    for copy in sent:
        copy.wait_send()


def body(tokens, routes, combine, gate_weight, up_weight, down_weight):
    info = jnp.concatenate([routes.astype(F32).T, combine.T, jnp.zeros((4, 16), F32)], axis=0)
    info = jnp.tile(info, (1, 8))
    vmem = pl.BlockSpec(memory_space=pltpu.VMEM)
    hbm = pl.BlockSpec(memory_space=pltpu.HBM)
    dma = pltpu.SemaphoreType.DMA
    part = (16, 32, CW)
    return pl.pallas_call(
        kernel,
        out_shape=jax.ShapeDtypeStruct((16, 4096), BF16),
        in_specs=[vmem, vmem, hbm, hbm, hbm],
        out_specs=vmem,
        scratch_shapes=[
            pltpu.VMEM((8, 16, CW), BF16),
            pltpu.VMEM((8, 8, 128), F32),
            pltpu.VMEM(part, BF16),
            pltpu.VMEM((8,) + part, BF16),
            pltpu.VMEM((4096, 512), BF16),
            pltpu.VMEM((4096, 512), BF16),
            pltpu.VMEM((512, 4096), BF16),
            pltpu.VMEM((512, 512), F32),
            pltpu.VMEM((512, 512), F32),
            pltpu.VMEM((512, 512), BF16),
            pltpu.VMEM((512, 128), BF16),
            pltpu.VMEM((128, 512), BF16),
            pltpu.VMEM((128, 512), BF16),
            pltpu.VMEM((4,) + part, BF16),
            pltpu.VMEM((4,) + part, BF16),
            pltpu.VMEM((4,) + part, BF16),
            pltpu.VMEM((4, 2, 32, CW), BF16),
            pltpu.VMEM((4, 2, 32, CW), BF16),
            pltpu.VMEM((4, 2, 32, CW), BF16),
            pltpu.VMEM((4, 2, 32, CW), BF16),
            pltpu.VMEM((4, 2, 2, 32, CW), BF16),
            pltpu.VMEM((4, 2, 2, 32, CW), BF16),
            pltpu.VMEM((4, 2, 2, 32, CW), BF16),
            pltpu.VMEM((4, 2, 2, 32, CW), BF16),
            pltpu.VMEM(part, BF16),
            pltpu.VMEM(part, BF16),
            pltpu.VMEM((8, 16, CW), BF16),
            pltpu.VMEM((8, 16, CW), BF16),
            dma((3,)),
            dma((8,)), dma((8,)), dma((8,)), dma((8,)),
            dma((16,)), dma((16,)),
            dma((9, 4)), dma((9, 4)),
            dma((4,)), dma((4,)),
            dma((6, 4)), dma((6, 4)),
            dma((16,)), dma((16,)),
            dma((8,)), dma((8,)),
        ],
        compiler_params=pltpu.CompilerParams(
            collective_id=0, has_side_effects=True, vmem_limit_bytes=60 * 1024 * 1024
        ),
        name="moe",
    )(tokens, info, gate_weight[0], up_weight[0], down_weight[0])


def solution(mesh):
    return jax.shard_map(
        body,
        mesh=mesh,
        in_specs=(
            P(("ep", "tp"), None),
            P(("ep", "tp"), None),
            P(("ep", "tp"), None),
            P("ep", None, "tp"),
            P("ep", None, "tp"),
            P("ep", "tp", None),
        ),
        out_specs=P(("ep", "tp"), None),
        check_vma=False,
    )
```

```python
import contextlib

import jax
import jax.numpy as jnp
from jax import lax
from jax.experimental import pallas as pl
from jax.experimental.pallas import tpu as pltpu
from jax.sharding import PartitionSpec as P

MESH = pl.DeviceIdType.MESH
PROFILE = False
F32 = jnp.float32
BF16 = jnp.bfloat16
NX, NY, NZ = 4, 4, 4
RW = 384
DW = 512
DIRECT = 8 * RW
HOPS = (
    (0, 0), (1, 1), (3, 3), (0, 2), (2, 2), (1, 3), (3, 1), (2, 0),
    (0, 1), (0, 3), (1, 0), (3, 0), (1, 2), (3, 2), (2, 1), (2, 3),
)
COPIES = 176


def scope(name):
    return jax.named_scope(name) if PROFILE else contextlib.nullcontext()


def kernel(
    tok_ref, info_ref, wg_hbm, wu_hbm, wd_hbm, out_ref,
    infos, t2, t1, p2, p1, x2, x1, wg, wu, wd, accg, accu, hid, sel, whi, wlo,
    part2, mate2, part1, mate1, far_s, far_r, near_s, near_r,
    fin2, fin1, r2, r1, o2s, o1s, o2r, o1r,
    w_sem, send_sems, recv_sems,
):
    ep = lax.axis_index("ep")
    tp = lax.axis_index("tp")
    y, z = ep // NZ, ep % NZ
    x, c = tp // 2, tp % 2
    sent = []

    def on_tp(other):
        return {"ep": ep, "tp": other}

    def on_ep(other):
        return {"ep": other, "tp": tp}

    def remote(src, dst, device):
        k = len(sent)
        copy = pltpu.make_async_remote_copy(
            src_ref=src, dst_ref=dst, send_sem=send_sems.at[k], recv_sem=recv_sems.at[k],
            device_id=device, device_id_type=MESH,
        )
        copy.start()
        sent.append(copy)
        return copy

    def arrived(copies):
        for copy in copies:
            copy.wait_recv()

    mate = x * 2 + (1 - c)
    right = ((x + 1) % NX) * 2 + c
    left = ((x + 3) % NX) * 2 + c
    far = ((x + 2) % NX) * 2 + c

    with scope("k00_barrier"):
        loads = []
        for n, (src, dst) in enumerate(((wg_hbm, wg), (wu_hbm, wu), (wd_hbm, wd))):
            load = pltpu.make_async_copy(src, dst, w_sem.at[n])
            load.start()
            loads.append(load)
        barrier = pltpu.get_barrier_semaphore()
        for j in range(1, 8):
            pl.semaphore_signal(barrier, inc=1, device_id=on_tp((tp + j) % 8), device_id_type=MESH)
        for dy in range(NY):
            for dz in range(NZ):
                if dy or dz:
                    other = ((y + dy) % NY) * NZ + (z + dz) % NZ
                    pl.semaphore_signal(barrier, inc=1, device_id=on_ep(other), device_id_type=MESH)
        pl.semaphore_wait(barrier, 22)

    def ring_cols(t):
        return pl.ds(pl.multiple_of(t * RW, 128), RW)

    def direct_cols(core):
        return pl.ds(pl.multiple_of(DIRECT + core * DW, 128), DW)

    with scope("k01_tsend"):
        offsets = (4, 5, 3, 2, 6, 7, 1)
        peers = [(tp + j) % 8 for j in offsets]
        got_info = [remote(info_ref, infos.at[tp], on_tp(t)) for t in peers]
        got_t2 = [remote(tok_ref.at[:, ring_cols(t)], t2.at[tp], on_tp(t)) for t in peers]
        got_t1 = [remote(tok_ref.at[:, direct_cols(t % 2)], t1.at[tp], on_tp(t)) for t in peers]
        infos[tp] = info_ref[...]
        t2[tp] = tok_ref[:, ring_cols(tp)]
        t1[tp] = tok_ref[:, direct_cols(c)]
    with scope("k02_iwait"):
        arrived(got_info)

    with scope("k03_sel"):
        lane8 = lax.broadcasted_iota(jnp.int32, (8, 128), 1) // 16
        info = jnp.zeros((8, 128), F32)
        for b in range(8):
            info = info + jnp.where(lane8 == b, infos[b], 0.0)
        row = lax.broadcasted_iota(jnp.int32, (512, 128), 0)
        lane = lax.broadcasted_iota(jnp.int32, (512, 128), 1)
        expert = (row // 32).astype(F32)
        slot = (row % 4).astype(F32)
        same = (lane // 16) == ((row % 32) // 4)
        first_of = jnp.where(info[0:1] == expert, 1.0, 0.0)
        second_of = jnp.where(info[1:2] == expert, 1.0, 0.0)
        named = first_of + second_of
        urow = lax.broadcasted_iota(jnp.int32, (128, 128), 0)
        ulane = lax.broadcasted_iota(jnp.int32, (128, 128), 1)
        before = jnp.where((urow < ulane) & ((urow // 16) == (ulane // 16)), 1.0, 0.0).astype(BF16)
        count = jnp.dot(named.astype(BF16), before, preferred_element_type=F32)
        hit = same & (count == slot)
        sel[...] = jnp.where(hit, named, 0.0).astype(BF16)

    with scope("k04_twait"):
        arrived(got_t2)

    def spread(picked, landing):
        copies = {}
        for n in (4, 1, 2, 3, 5, 6, 7, 12, 13, 14, 15, 8, 9, 10, 11):
            dy, dz = HOPS[n]
            other = ((y + dy) % NY) * NZ + (z + dz) % NZ
            copies[n] = remote(picked.at[other], landing.at[n // 8, n % 8], on_ep(other))
        return copies

    def of_half(copies, h):
        return [copy for n, copy in copies.items() if n // 8 == h]

    with scope("k05_pick2"):
        picked = jnp.dot(sel[...], t2[...].reshape(128, RW), preferred_element_type=F32)
        p2[...] = picked.astype(BF16).reshape(16, 32, RW)
        x2[tp, 0, 0] = p2[ep]
        spread2 = spread(p2, x2.at[tp])
    with scope("k06_pick1"):
        arrived(got_t1)
        picked = jnp.dot(sel[...], t1[...].reshape(128, DW), preferred_element_type=F32)
        p1[...] = picked.astype(BF16).reshape(16, 32, DW)
        x1[c, 0, 0] = p1[ep]
    with scope("k07_weights"):
        weight = jnp.where(hit, first_of * info[2:3] + second_of * info[3:4], 0.0).T
        high = weight.astype(BF16)
        whi[...] = high
        wlo[...] = (weight - high.astype(F32)).astype(BF16)

    LO, HI, ALL = pl.ds(0, 4), pl.ds(4, 4), pl.ds(0, 8)

    def push(t, h, rows, device):
        block = x2.at[t, h, rows]
        return remote(block, block, on_tp(device))

    def half_state():
        return {}

    st = [half_state(), half_state()]

    def own_first(h):
        s = st[h]
        s["r_lo"] = push(tp, h, LO, right)
        s["l_hi"] = push(tp, h, HI, left)
        s["m_own"] = push(tp, h, ALL, mate)

    def own_second(h):
        s = st[h]
        s["r_hi"] = push(tp, h, HI, right)
        s["l_lo"] = push(tp, h, LO, left)

    def forward(h):
        s = st[h]
        s["r_lo"].wait_recv()
        s["f_lo"] = push(left, h, LO, right)
        s["m_left_lo"] = push(left, h, LO, mate)
        s["l_hi"].wait_recv()
        s["f_hi"] = push(right, h, HI, left)
        s["m_right_hi"] = push(right, h, HI, mate)

    def near_rest(h):
        s = st[h]
        s["r_hi"].wait_recv()
        s["m_left_hi"] = push(left, h, HI, mate)
        s["l_lo"].wait_recv()
        s["m_right_lo"] = push(right, h, LO, mate)

    def far_rest(h):
        s = st[h]
        s["f_lo"].wait_recv()
        s["m_far_lo"] = push(far, h, LO, mate)
        s["f_hi"].wait_recv()
        s["m_far_hi"] = push(far, h, HI, mate)

    spread1 = {}

    def direct_share(h):
        arrived(of_half(spread1, h))
        block = x1.at[c, h]
        st[h]["m_direct"] = remote(block, block, on_tp(mate))

    def accumulate(h, a, rows, fresh):
        gate = jnp.dot(a, wg[rows, :], preferred_element_type=F32)
        up = jnp.dot(a, wu[rows, :], preferred_element_type=F32)
        if fresh:
            accg[h] = gate
            accu[h] = up
        else:
            accg[h] += gate
            accu[h] += up

    def gate_up(h, k, names):
        arrived([st[h][name] for name in names])
        chip = (x + k) % NX
        a = jnp.concatenate(
            [x2[chip * 2, h].reshape(256, RW), x2[chip * 2 + 1, h].reshape(256, RW)], axis=1
        )
        accumulate(h, a, pl.ds(pl.multiple_of(chip * 2 * RW, 256), 2 * RW), k == 0)

    def gate_up_direct(h):
        st[h]["m_direct"].wait_recv()
        a = jnp.concatenate([x1[0, h].reshape(256, DW), x1[1, h].reshape(256, DW)], axis=1)
        accumulate(h, a, pl.ds(DIRECT, 2 * DW), False)

    def silu(h):
        gate = accg[h]
        hid[h] = (gate / (1.0 + jnp.exp(-gate)) * accu[h]).astype(BF16)

    def down(h, k):
        chip = (x + k) % NX
        cols = pl.ds(pl.multiple_of(chip * 2 * RW, 256), 2 * RW)
        part = jnp.dot(hid[h], wd[:, cols], preferred_element_type=F32).astype(BF16)
        part2[h, k, 0] = part[:, :RW].reshape(8, 32, RW)
        part2[h, k, 1] = part[:, RW:].reshape(8, 32, RW)
        st[h]["pair", k] = remote(part2.at[h, k, 1 - c], mate2.at[h, k], on_tp(mate))

    def down_direct(h):
        part = jnp.dot(hid[h], wd[:, DIRECT:], preferred_element_type=F32).astype(BF16)
        part1[h, 0] = part[:, :DW].reshape(8, 32, DW)
        part1[h, 1] = part[:, DW:].reshape(8, 32, DW)
        st[h]["pair_direct"] = remote(part1.at[h, 1 - c], mate1.at[h], on_tp(mate))

    def chip_sum(h, k, start):
        return part2[h, k, c, start:start + 4].astype(F32) + mate2[h, k, start:start + 4].astype(F32)

    def reduce_far(h):
        st[h]["pair", 2].wait_recv()
        far_s[h, 0] = chip_sum(h, 2, 0).astype(BF16)
        st[h]["far_lo"] = remote(far_s.at[h, 0], far_r.at[h, 0], on_tp(right))
        far_s[h, 1] = chip_sum(h, 2, 4).astype(BF16)
        st[h]["far_hi"] = remote(far_s.at[h, 1], far_r.at[h, 1], on_tp(left))

    def reduce_near_first(h):
        st[h]["pair", 1].wait_recv()
        near_s[h, 0, 1] = chip_sum(h, 1, 4).astype(BF16)
        st[h]["near_r_hi"] = remote(near_s.at[h, 0, 1], near_r.at[h, 0, 1], on_tp(right))
        st[h]["pair", 3].wait_recv()
        near_s[h, 1, 0] = chip_sum(h, 3, 0).astype(BF16)
        st[h]["near_l_lo"] = remote(near_s.at[h, 1, 0], near_r.at[h, 1, 0], on_tp(left))

    def reduce_near_second(h):
        st[h]["far_lo"].wait_recv()
        near_s[h, 0, 0] = (chip_sum(h, 1, 0) + far_r[h, 0].astype(F32)).astype(BF16)
        st[h]["near_r_lo"] = remote(near_s.at[h, 0, 0], near_r.at[h, 0, 0], on_tp(right))
        st[h]["far_hi"].wait_recv()
        near_s[h, 1, 1] = (chip_sum(h, 3, 4) + far_r[h, 1].astype(F32)).astype(BF16)
        st[h]["near_l_hi"] = remote(near_s.at[h, 1, 1], near_r.at[h, 1, 1], on_tp(left))

    back2, back1 = [], []

    def give_back(h, start, stop, fin, landing, copies):
        for j in range(start, stop):
            dy, dz = HOPS[h * 8 + j]
            if dy or dz:
                other = ((y + NY - dy) % NY) * NZ + (z + NZ - dz) % NZ
                copies.append(remote(fin.at[h, j], landing.at[ep], on_ep(other)))
            else:
                landing[ep] = fin[h, j]

    def reduce_last(h):
        s = st[h]
        s["pair", 0].wait_recv()
        arrived([s["near_r_hi"], s["near_l_hi"]])
        total = chip_sum(h, 0, 4) + near_r[h, 0, 1].astype(F32) + near_r[h, 1, 1].astype(F32)
        fin2[h, 4:8] = total.astype(BF16)
        give_back(h, 4, 8, fin2, r2, back2)
        arrived([s["near_r_lo"], s["near_l_lo"]])
        total = chip_sum(h, 0, 0) + near_r[h, 0, 0].astype(F32) + near_r[h, 1, 0].astype(F32)
        fin2[h, 0:4] = total.astype(BF16)
        give_back(h, 0, 4, fin2, r2, back2)

    def direct_back(h):
        st[h]["pair_direct"].wait_recv()
        fin1[h] = (part1[h, c].astype(F32) + mate1[h].astype(F32)).astype(BF16)
        give_back(h, 0, 8, fin1, r1, back1)

    A, B = 0, 1
    LEFT = ("m_left_lo", "m_left_hi")
    RIGHT = ("m_right_lo", "m_right_hi")
    FAR = ("m_far_lo", "m_far_hi")
    with scope("k10_ownA"):
        arrived(of_half(spread2, A))
        own_first(A)
        own_second(A)
    with scope("k11_ownB1"):
        arrived(of_half(spread2, B))
        own_first(B)
        spread1.update(spread(p1, x1.at[c]))
    with scope("k12_guA_own"):
        loads[0].wait()
        loads[1].wait()
        gate_up(A, 0, ("m_own",))
    with scope("k13_fwdA"):
        forward(A)
    with scope("k14_nearA"):
        own_second(B)
        near_rest(A)
    with scope("k15_guB_own"):
        gate_up(B, 0, ("m_own",))
    with scope("k16_fwdB"):
        forward(B)
    with scope("k17_farA"):
        far_rest(A)
    with scope("k18_guA_lr"):
        gate_up(A, 3, LEFT)
        gate_up(A, 1, RIGHT)
    with scope("k19_directA"):
        direct_share(A)
    with scope("k20_guA_far"):
        gate_up(A, 2, FAR)
    with scope("k21_guA_d"):
        gate_up_direct(A)
    with scope("k22_downA21"):
        silu(A)
        loads[2].wait()
        down(A, 2)
        down(A, 1)
    with scope("k23_nearB"):
        near_rest(B)
    with scope("k24_directB"):
        direct_share(B)
    with scope("k25_rfarA"):
        reduce_far(A)
    with scope("k26_downA30d"):
        down(A, 3)
        down(A, 0)
        down_direct(A)
    with scope("k27_rnear1A"):
        reduce_near_first(A)
    with scope("k28_farB"):
        far_rest(B)
    with scope("k29_guB_lr"):
        gate_up(B, 3, LEFT)
        gate_up(B, 1, RIGHT)
    with scope("k30_guB_d"):
        gate_up_direct(B)
    with scope("k31_rnear2A"):
        reduce_near_second(A)
    with scope("k32_dbackA"):
        direct_back(A)
    with scope("k33_guB_far"):
        gate_up(B, 2, FAR)
    with scope("k34_downB21"):
        silu(B)
        down(B, 2)
        down(B, 1)
    with scope("k35_rfarB"):
        reduce_far(B)
    with scope("k36_downB30d"):
        down(B, 3)
        down(B, 0)
        down_direct(B)
    with scope("k37_rnear1B"):
        reduce_near_first(B)
    with scope("k38_rlastA"):
        reduce_last(A)
    with scope("k39_dbackB"):
        direct_back(B)
    with scope("k40_rnear2B"):
        reduce_near_second(B)
    with scope("k41_rlastB"):
        reduce_last(B)

    def weighted(landing, width, out):
        rows = landing[...].reshape(512, width)
        total = jnp.dot(whi[...], rows, preferred_element_type=F32)
        total = total + jnp.dot(wlo[...], rows, preferred_element_type=F32)
        out[...] = total.astype(BF16).reshape(8, 16, width)

    with scope("k42_comb1"):
        arrived(back1)
        weighted(r1, DW, o1s)
        got_o1 = [remote(o1s.at[t], o1r.at[tp], on_tp(t)) for t in peers]
        o1r[tp] = o1s[tp]
    with scope("k44_backwait"):
        arrived(back2)
    with scope("k45_comb2"):
        weighted(r2, RW, o2s)
        got_o2 = [remote(o2s.at[t], o2r.at[tp], on_tp(t)) for t in peers]
        o2r[tp] = o2s[tp]
    with scope("k46_o1"):
        arrived(got_o1)
        for core in range(2):
            total = o1r[core].astype(F32)
            for chip in range(1, NX):
                total = total + o1r[chip * 2 + core].astype(F32)
            out_ref[:, DIRECT + core * DW:DIRECT + (core + 1) * DW] = total.astype(BF16)
    with scope("k47_o2"):
        arrived(got_o2)
    with scope("k48_store"):
        for t in range(8):
            out_ref[:, t * RW:(t + 1) * RW] = o2r[t]
        for copy in sent:
            copy.wait_send()


def body(tokens, routes, combine, gate_weight, up_weight, down_weight):
    info = jnp.concatenate([routes.astype(F32).T, combine.T, jnp.zeros((4, 16), F32)], axis=0)
    info = jnp.tile(info, (1, 8))
    vmem = pl.BlockSpec(memory_space=pltpu.VMEM)
    hbm = pl.BlockSpec(memory_space=pltpu.HBM)
    dma = pltpu.SemaphoreType.DMA
    return pl.pallas_call(
        kernel,
        out_shape=jax.ShapeDtypeStruct((16, 4096), BF16),
        in_specs=[vmem, vmem, hbm, hbm, hbm],
        out_specs=vmem,
        scratch_shapes=[
            pltpu.VMEM((8, 8, 128), F32),
            pltpu.VMEM((8, 16, RW), BF16),
            pltpu.VMEM((8, 16, DW), BF16),
            pltpu.VMEM((16, 32, RW), BF16),
            pltpu.VMEM((16, 32, DW), BF16),
            pltpu.VMEM((8, 2, 8, 32, RW), BF16),
            pltpu.VMEM((2, 2, 8, 32, DW), BF16),
            pltpu.VMEM((4096, 512), BF16),
            pltpu.VMEM((4096, 512), BF16),
            pltpu.VMEM((512, 4096), BF16),
            pltpu.VMEM((2, 256, 512), F32),
            pltpu.VMEM((2, 256, 512), F32),
            pltpu.VMEM((2, 256, 512), BF16),
            pltpu.VMEM((512, 128), BF16),
            pltpu.VMEM((128, 512), BF16),
            pltpu.VMEM((128, 512), BF16),
            pltpu.VMEM((2, 4, 2, 8, 32, RW), BF16),
            pltpu.VMEM((2, 4, 8, 32, RW), BF16),
            pltpu.VMEM((2, 2, 8, 32, DW), BF16),
            pltpu.VMEM((2, 8, 32, DW), BF16),
            pltpu.VMEM((2, 2, 4, 32, RW), BF16),
            pltpu.VMEM((2, 2, 4, 32, RW), BF16),
            pltpu.VMEM((2, 2, 2, 4, 32, RW), BF16),
            pltpu.VMEM((2, 2, 2, 4, 32, RW), BF16),
            pltpu.VMEM((2, 8, 32, RW), BF16),
            pltpu.VMEM((2, 8, 32, DW), BF16),
            pltpu.VMEM((16, 32, RW), BF16),
            pltpu.VMEM((16, 32, DW), BF16),
            pltpu.VMEM((8, 16, RW), BF16),
            pltpu.VMEM((8, 16, DW), BF16),
            pltpu.VMEM((8, 16, RW), BF16),
            pltpu.VMEM((8, 16, DW), BF16),
            dma((3,)),
            dma((COPIES,)),
            dma((COPIES,)),
        ],
        compiler_params=pltpu.CompilerParams(
            collective_id=0, has_side_effects=True, vmem_limit_bytes=60 * 1024 * 1024
        ),
        name="moe",
    )(tokens, info, gate_weight[0], up_weight[0], down_weight[0])


def solution(mesh):
    return jax.shard_map(
        body,
        mesh=mesh,
        in_specs=(
            P(("ep", "tp"), None),
            P(("ep", "tp"), None),
            P(("ep", "tp"), None),
            P("ep", None, "tp"),
            P("ep", None, "tp"),
            P("ep", "tp", None),
        ),
        out_specs=P(("ep", "tp"), None),
        check_vma=False,
    )
```

```python
from typing import Any, NamedTuple

import jax
import jax.numpy as jnp
from jax import lax
from jax.experimental import pallas as pl
from jax.experimental.pallas import tpu as pltpu
from jax.sharding import PartitionSpec as P

MESH = pl.DeviceIdType.MESH
F32 = jnp.float32
BF16 = jnp.bfloat16
NX, NY, NZ = 4, 4, 4
A, B = 0, 1
RING = (384, 256)
DIRECT = (512, 1024)
RECVS = 57
TALLY = 1024


def hop(h, j):
    dy = j // 2
    return dy, (2 * (j % 2) + dy + h) % NZ


class Half(NamedTuple):
    t2: Any
    t1: Any
    p2: Any
    p1: Any
    x2: Any
    x1: Any
    accg: Any
    accu: Any
    hid: Any
    part2: Any
    mate2: Any
    part1: Any
    mate1: Any
    far_s: Any
    far_r: Any
    near_s: Any
    near_r: Any
    fin2: Any
    fin1: Any
    r2: Any
    r1: Any
    o2s: Any
    o1s: Any
    o2r: Any
    o1r: Any


def half_scratch(h):
    r, d = RING[h], DIRECT[h]
    bf = lambda *shape: pltpu.VMEM(shape, BF16)
    f = lambda *shape: pltpu.VMEM(shape, F32)
    return Half(
        t2=bf(8, 16, r), t1=bf(8, 16, d), p2=bf(8, 32, r), p1=bf(8, 32, d),
        x2=bf(8, 8, 32, r), x1=bf(2, 8, 32, d),
        accg=f(256, 512), accu=f(256, 512), hid=bf(256, 512),
        part2=bf(4, 2, 8, 32, r), mate2=bf(4, 8, 32, r), part1=bf(2, 8, 32, d), mate1=bf(8, 32, d),
        far_s=bf(2, 4, 32, r), far_r=bf(2, 4, 32, r), near_s=bf(2, 2, 4, 32, r), near_r=bf(2, 2, 4, 32, r),
        fin2=bf(8, 32, r), fin1=bf(8, 32, d), r2=bf(8, 32, r), r1=bf(8, 32, d),
        o2s=bf(8, 16, r), o1s=bf(8, 16, d), o2r=bf(8, 16, r), o1r=bf(8, 16, d),
    )


def kernel(
    tok_hbm, routes_hbm, combine_hbm, wg_hbm, wu_hbm, wd_hbm, out_ref,
    tok_ref, routes_ref, combine_ref, info_ref, infos, wg, wu, wd, sel, whi, wlo, tally, expert_of, slot_of, before,
    w_sem, send_sems, recv_sems, *halves,
):
    half = [Half(*halves[:len(Half._fields)]), Half(*halves[len(Half._fields):])]
    ep = lax.axis_index("ep")
    tp = lax.axis_index("tp")
    y, z = ep // NZ, ep % NZ
    x, c = tp // 2, tp % 2
    recv_of = {}
    sent = [0, 0, 0, 0]

    def on_tp(other):
        return {"ep": ep, "tp": other}

    def on_ep(other):
        return {"ep": other, "tp": tp}

    def recv_sem(name):
        return recv_sems.at[recv_of.setdefault(name, len(recv_of))]

    def remote(group, name, src, dst, device):
        size = src.dtype.itemsize
        for dim in src.shape:
            size *= dim
        sent[group] += size // 4096
        pltpu.make_async_remote_copy(
            src_ref=src, dst_ref=dst, send_sem=send_sems.at[group], recv_sem=recv_sem(name),
            device_id=device, device_id_type=MESH,
        ).start()

    def arrived(name, like):
        pltpu.make_async_remote_copy(
            src_ref=like, dst_ref=like, send_sem=send_sems.at[0], recv_sem=recv_sem(name),
            device_id=on_tp(mate), device_id_type=MESH,
        ).wait_recv()

    mate = x * 2 + (1 - c)
    right = ((x + 1) % NX) * 2 + c
    left = ((x + 3) % NX) * 2 + c
    far = ((x + 2) % NX) * 2 + c

    small = []
    for n, (src, dst) in enumerate(
        ((routes_hbm, routes_ref), (combine_hbm, combine_ref), (tok_hbm, tok_ref))
    ):
        load = pltpu.make_async_copy(src, dst, w_sem.at[3 + n])
        load.start()
        small.append(load)
    barrier = pltpu.get_barrier_semaphore()
    for j in range(1, 8):
        pl.semaphore_signal(barrier, inc=1, device_id=on_tp((tp + j) % 8), device_id_type=MESH)
    for dy in range(NY):
        for dz in range(NZ):
            if dy or dz:
                other = ((y + dy) % NY) * NZ + (z + dz) % NZ
                pl.semaphore_signal(barrier, inc=1, device_id=on_ep(other), device_id_type=MESH)
    small[0].wait()
    small[1].wait()
    info_ref[0:2, :] = jnp.concatenate([routes_ref[...].astype(F32)] * 8, axis=1)
    info_ref[2:4, :] = jnp.concatenate([combine_ref[...]] * 8, axis=1)
    info_ref[4:8, :] = jnp.zeros((4, 128), F32)
    small[2].wait()
    pl.semaphore_wait(barrier, 22)

    def ring_cols(h, t):
        return pl.ds(pl.multiple_of(t * RING[h], 128), RING[h])

    def direct_cols(h, core):
        return pl.ds(pl.multiple_of(8 * RING[h] + core * DIRECT[h], 128), DIRECT[h])

    peers = [(tp + j) % 8 for j in (4, 5, 3, 2, 6, 7, 1)]
    for t in peers:
        remote(0, "info", info_ref, infos.at[tp], on_tp(t))
    for h in (A, B):
        for t in peers:
            remote(0, ("t2", h), tok_ref.at[:, ring_cols(h, t)], half[h].t2.at[tp], on_tp(t))
    infos[tp] = info_ref[...]
    for h in (A, B):
        half[h].t2[tp] = tok_ref[:, ring_cols(h, tp)]
        half[h].t1[tp] = tok_ref[:, direct_cols(h, c)]
    loads = []
    for n, (src, dst) in enumerate(((wg_hbm, wg), (wu_hbm, wu), (wd_hbm, wd))):
        load = pltpu.make_async_copy(src, dst, w_sem.at[n])
        load.start()
        loads.append(load)
    row = lax.broadcasted_iota(jnp.int32, (512, 128), 0)
    lane = lax.broadcasted_iota(jnp.int32, (512, 128), 1)
    j_of = (row // 32) % 8
    dy_of = j_of // 2
    dz_of = (2 * (j_of % 2) + dy_of + row // 256) % NZ
    expert_of[...] = (((y + dy_of) % NY) * NZ + (z + dz_of) % NZ).astype(F32)
    same = (lane // 16) == ((row % 32) // 4)
    slot_of[...] = jnp.where(same, row % 4, 128).astype(F32)
    urow = lax.broadcasted_iota(jnp.int32, (128, 128), 0)
    ulane = lax.broadcasted_iota(jnp.int32, (128, 128), 1)
    before[...] = jnp.where((urow < ulane) & ((urow // 16) == (ulane // 16)), 1.0, 0.0).astype(BF16)
    arrived("info", infos.at[pl.ds(0, 7)])
    for h in (A, B):
        for t in peers:
            remote(0, ("t1", h), tok_ref.at[:, direct_cols(h, t % 2)], half[h].t1.at[tp], on_tp(t))

    lane8 = lax.broadcasted_iota(jnp.int32, (8, 128), 1) // 16
    info = jnp.zeros((8, 128), F32)
    for b in range(8):
        info = info + jnp.where(lane8 == b, infos[b], 0.0)
    expert = expert_of[...]
    first_of = jnp.where(info[0:1] == expert, 1.0, 0.0)
    second_of = jnp.where(info[1:2] == expert, 1.0, 0.0)
    named = first_of + second_of
    count = jnp.dot(named.astype(BF16), before[...], preferred_element_type=F32)
    hit = count == slot_of[...]
    sel[...] = jnp.where(hit, named, 0.0).astype(BF16)

    def pick(h, tokens, width, picked, landing, name):
        rows = sel[h * 256:(h + 1) * 256]
        got = jnp.dot(rows, tokens[...].reshape(128, width), preferred_element_type=F32)
        picked[...] = got.astype(BF16).reshape(8, 32, width)
        order = (4, 5, 6, 7, 2, 3, 1, 0) if h == A else (4, 5, 6, 2, 3, 7, 0, 1)
        for j in order:
            dy, dz = hop(h, j)
            if dy or dz:
                other = ((y + dy) % NY) * NZ + (z + dz) % NZ
                remote(0, (name, h), picked.at[j], landing.at[j], on_ep(other))
            else:
                landing[j] = picked[j]

    def others(h):
        return pl.ds(0, 7 if h == A else 8)

    def pick_ring(h):
        arrived(("t2", h), half[h].t2.at[pl.ds(0, 7)])
        pick(h, half[h].t2, RING[h], half[h].p2, half[h].x2.at[tp], "spread2")

    def pick_direct(h):
        arrived(("t1", h), half[h].t1.at[pl.ds(0, 7)])
        pick(h, half[h].t1, DIRECT[h], half[h].p1, half[h].x1.at[c], "spread1")

    pick_ring(A)
    pick_ring(B)
    weight = jnp.where(hit, first_of * info[2:3] + second_of * info[3:4], 0.0).T
    high = weight.astype(BF16)
    whi[...] = high
    wlo[...] = (weight - high.astype(F32)).astype(BF16)

    LO, HI, ALL = pl.ds(0, 4), pl.ds(4, 4), pl.ds(0, 8)

    def push(name, t, h, rows, device):
        block = half[h].x2.at[t, rows]
        remote(1, (name, h), block, block, on_tp(device))

    def got(name, h, rows):
        arrived((name, h), half[h].x2.at[0, rows])

    def own_first(h):
        push("m_own", tp, h, ALL, mate)
        push("r_lo", tp, h, LO, right)
        push("l_hi", tp, h, HI, left)

    def own_second(h):
        push("r_hi", tp, h, HI, right)
        push("l_lo", tp, h, LO, left)

    def forward(h):
        got("r_lo", h, LO)
        push("m_left", left, h, LO, mate)
        push("f_lo", left, h, LO, right)
        got("l_hi", h, HI)
        push("m_right", right, h, HI, mate)
        push("f_hi", right, h, HI, left)

    def near_rest(h):
        got("r_hi", h, HI)
        push("m_left", left, h, HI, mate)
        got("l_lo", h, LO)
        push("m_right", right, h, LO, mate)

    def far_rest(h):
        got("f_lo", h, LO)
        push("m_far", far, h, LO, mate)
        got("f_hi", h, HI)
        push("m_far", far, h, HI, mate)

    def direct_share(h):
        x1 = half[h].x1
        arrived(("spread1", h), x1.at[0, others(h)])
        remote(1, ("m_direct", h), x1.at[c], x1.at[c], on_tp(mate))

    def accumulate(h, a, rows, fresh):
        gate = jnp.dot(a, wg[rows, :], preferred_element_type=F32)
        up = jnp.dot(a, wu[rows, :], preferred_element_type=F32)
        if fresh:
            half[h].accg[...] = gate
            half[h].accu[...] = up
        else:
            half[h].accg[...] += gate
            half[h].accu[...] += up

    def gate_up(h, k, name):
        got(name, h, ALL)
        chip = (x + k) % NX
        x2, r = half[h].x2, RING[h]
        a = jnp.concatenate([x2[chip * 2].reshape(256, r), x2[chip * 2 + 1].reshape(256, r)], axis=1)
        accumulate(h, a, pl.ds(pl.multiple_of(chip * 2 * r, 256), 2 * r), k == 0)

    def gate_up_direct(h):
        x1, d = half[h].x1, DIRECT[h]
        arrived(("m_direct", h), x1.at[0])
        a = jnp.concatenate([x1[0].reshape(256, d), x1[1].reshape(256, d)], axis=1)
        accumulate(h, a, pl.ds(8 * RING[h], 2 * d), False)

    def silu(h):
        gate = half[h].accg[...]
        half[h].hid[...] = (gate / (1.0 + jnp.exp(-gate)) * half[h].accu[...]).astype(BF16)

    def down(h, *ks):
        s, r = half[h], RING[h]
        parts = []
        for k in ks:
            cols = pl.ds(pl.multiple_of(((x + k) % NX) * 2 * r, 256), 2 * r)
            parts.append(jnp.dot(s.hid[...], wd[:, cols], preferred_element_type=F32).astype(BF16))
        for k, part in zip(ks, parts):
            s.part2[k, 0] = part[:, :r].reshape(8, 32, r)
            s.part2[k, 1] = part[:, r:].reshape(8, 32, r)
        for k in ks:
            remote(2, ("pair", h, k), s.part2.at[k, 1 - c], s.mate2.at[k], on_tp(mate))

    def down_direct(h):
        s, d = half[h], DIRECT[h]
        for core in range(2):
            cols = pl.ds(8 * RING[h] + core * d, d)
            part = jnp.dot(s.hid[...], wd[:, cols], preferred_element_type=F32).astype(BF16)
            s.part1[core] = part.reshape(8, 32, d)
        remote(2, ("pair_direct", h), s.part1.at[1 - c], s.mate1, on_tp(mate))

    def paired(h, k):
        arrived(("pair", h, k), half[h].mate2.at[k])

    def chip_sum(h, k, start):
        s = half[h]
        return s.part2[k, c, start:start + 4].astype(F32) + s.mate2[k, start:start + 4].astype(F32)

    def reduce_far(h):
        s = half[h]
        paired(h, 2)
        s.far_s[0] = chip_sum(h, 2, 0).astype(BF16)
        remote(2, ("far_lo", h), s.far_s.at[0], s.far_r.at[0], on_tp(right))
        s.far_s[1] = chip_sum(h, 2, 4).astype(BF16)
        remote(2, ("far_hi", h), s.far_s.at[1], s.far_r.at[1], on_tp(left))

    def near_send(h, side, rows, value):
        s = half[h]
        s.near_s[side, rows] = value.astype(BF16)
        name = ("near_hi" if rows else "near_lo", h)
        remote(2, name, s.near_s.at[side, rows], s.near_r.at[side, rows], on_tp((right, left)[side]))

    def reduce_near_first(h):
        paired(h, 1)
        near_send(h, 0, 1, chip_sum(h, 1, 4))
        paired(h, 3)
        near_send(h, 1, 0, chip_sum(h, 3, 0))

    def reduce_near_second(h):
        s = half[h]
        arrived(("far_lo", h), s.far_r.at[0])
        near_send(h, 0, 0, chip_sum(h, 1, 0) + s.far_r[0].astype(F32))
        arrived(("far_hi", h), s.far_r.at[1])
        near_send(h, 1, 1, chip_sum(h, 3, 4) + s.far_r[1].astype(F32))

    def give_back(h, blocks, fin, landing, name):
        for j in blocks:
            dy, dz = hop(h, j)
            if dy or dz:
                other = ((y + NY - dy) % NY) * NZ + (z + NZ - dz) % NZ
                remote(3, (name, h), fin.at[j], landing.at[j], on_ep(other))
            else:
                landing[j] = fin[j]

    def reduce_last(h):
        s = half[h]
        paired(h, 0)
        near_r = s.near_r
        for rows, name in ((1, "near_hi"), (0, "near_lo")):
            arrived((name, h), near_r.at[0])
            total = chip_sum(h, 0, rows * 4)
            total = total + near_r[0, rows].astype(F32) + near_r[1, rows].astype(F32)
            s.fin2[rows * 4:rows * 4 + 4] = total.astype(BF16)
            give_back(h, range(rows * 4, rows * 4 + 4), s.fin2, s.r2, "back2")

    def direct_back(h):
        s = half[h]
        arrived(("pair_direct", h), s.mate1)
        s.fin1[...] = (s.part1[c].astype(F32) + s.mate1[...].astype(F32)).astype(BF16)
        give_back(h, (4, 5, 6, 7, 2, 3, 0, 1), s.fin1, s.r1, "back1")

    def weigh(h, name, landing, width, out, everywhere):
        arrived((name, h), landing.at[others(h)])
        rows = landing[...].reshape(256, width)
        cols = slice(h * 256, (h + 1) * 256)
        total = jnp.dot(whi[:, cols], rows, preferred_element_type=F32)
        total = total + jnp.dot(wlo[:, cols], rows, preferred_element_type=F32)
        out[...] = total.astype(BF16).reshape(8, 16, width)
        for t in peers:
            remote(3, (name, "out", h), out.at[t], everywhere.at[tp], on_tp(t))
        everywhere[tp] = out[tp]

    def weigh_ring(h):
        weigh(h, "back2", half[h].r2, RING[h], half[h].o2s, half[h].o2r)

    def weigh_direct(h):
        weigh(h, "back1", half[h].r1, DIRECT[h], half[h].o1s, half[h].o1r)

    arrived(("spread2", A), half[A].x2.at[0, others(A)])
    own_first(A)
    own_second(A)
    pick_direct(A)
    pick_direct(B)
    loads[0].wait()
    loads[1].wait()
    gate_up(A, 0, "m_own")
    arrived(("spread2", B), half[B].x2.at[0, others(B)])
    forward(A)
    own_first(B)
    own_second(B)
    near_rest(A)
    gate_up(B, 0, "m_own")
    gate_up(A, 3, "m_left")
    gate_up(A, 1, "m_right")
    direct_share(A)
    far_rest(A)
    forward(B)
    gate_up_direct(A)
    gate_up(A, 2, "m_far")
    silu(A)
    loads[2].wait()
    down(A, 2)
    down_direct(A)
    near_rest(B)
    reduce_far(A)
    down(A, 1, 3)
    direct_share(B)
    gate_up(B, 3, "m_left")
    gate_up(B, 1, "m_right")
    far_rest(B)
    direct_back(A)
    reduce_near_first(A)
    gate_up_direct(B)
    gate_up(B, 2, "m_far")
    silu(B)
    down(B, 2)
    down_direct(B)
    reduce_near_second(A)
    reduce_far(B)
    down(B, 1, 3)
    direct_back(B)
    reduce_near_first(B)
    down(A, 0)
    down(B, 0)
    reduce_near_second(B)
    reduce_last(A)
    reduce_last(B)
    weigh_direct(A)
    weigh_direct(B)
    weigh_ring(A)
    weigh_ring(B)
    totals = []
    for h in (A, B):
        s = half[h]
        arrived(("back1", "out", h), s.o1r.at[pl.ds(0, 7)])
        arrived(("back2", "out", h), s.o2r.at[pl.ds(0, 7)])
    for h in (A, B):
        s = half[h]
        pieces = [s.o2r[t].astype(F32) for t in range(8)]
        for core in range(2):
            piece = s.o1r[core].astype(F32)
            for chip in range(1, NX):
                piece = piece + s.o1r[chip * 2 + core].astype(F32)
            pieces.append(piece)
        totals.append(jnp.concatenate(pieces, axis=1))
    out_ref[...] = (totals[0] + totals[1]).astype(BF16)
    for group in range(4):
        every = tally.at[pl.ds(0, sent[group])]
        pltpu.make_async_remote_copy(
            src_ref=every, dst_ref=every, send_sem=send_sems.at[group], recv_sem=recv_sems.at[0],
            device_id=on_tp(mate), device_id_type=MESH,
        ).wait_send()
    assert len(recv_of) == RECVS, len(recv_of)


def body(tokens, routes, combine, gate_weight, up_weight, down_weight):
    vmem = pl.BlockSpec(memory_space=pltpu.VMEM)
    hbm = pl.BlockSpec(memory_space=pltpu.HBM)
    dma = pltpu.SemaphoreType.DMA
    return pl.pallas_call(
        kernel,
        out_shape=jax.ShapeDtypeStruct((16, 4096), BF16),
        in_specs=[hbm] * 6,
        out_specs=vmem,
        scratch_shapes=[
            pltpu.VMEM((16, 4096), BF16),
            pltpu.VMEM((2, 16), jnp.int32),
            pltpu.VMEM((2, 16), F32),
            pltpu.VMEM((8, 128), F32),
            pltpu.VMEM((8, 8, 128), F32),
            pltpu.VMEM((4096, 512), BF16),
            pltpu.VMEM((4096, 512), BF16),
            pltpu.VMEM((512, 4096), BF16),
            pltpu.VMEM((512, 128), BF16),
            pltpu.VMEM((128, 512), BF16),
            pltpu.VMEM((128, 512), BF16),
            pltpu.VMEM((TALLY, 8, 128), F32),
            pltpu.VMEM((512, 128), F32),
            pltpu.VMEM((512, 128), F32),
            pltpu.VMEM((128, 128), BF16),
            dma((6,)),
            dma((4,)),
            dma((RECVS,)),
            *half_scratch(A),
            *half_scratch(B),
        ],
        compiler_params=pltpu.CompilerParams(
            collective_id=0, has_side_effects=True, vmem_limit_bytes=60 * 1024 * 1024
        ),
        name="moe",
    )(tokens, routes.T, combine.T, gate_weight[0], up_weight[0], down_weight[0])


def solution(mesh):
    return jax.shard_map(
        body,
        mesh=mesh,
        in_specs=(
            P(("ep", "tp"), None),
            P(("ep", "tp"), None),
            P(("ep", "tp"), None),
            P("ep", None, "tp"),
            P("ep", None, "tp"),
            P("ep", "tp", None),
        ),
        out_specs=P(("ep", "tp"), None),
        check_vma=False,
    )
```

```python
from typing import Any, NamedTuple

import jax
import jax.numpy as jnp
from jax import lax
from jax.experimental import pallas as pl
from jax.experimental.pallas import tpu as pltpu
from jax.sharding import PartitionSpec as P

MESH = pl.DeviceIdType.MESH
F32 = jnp.float32
BF16 = jnp.bfloat16
NX, NY, NZ = 4, 4, 4
A, B = 0, 1
RING = (256, 384)
DIRECT = (1024, 512)
RECVS = 59
TALLY = 1024


def hop(h, j):
    dy = j // 2
    return dy, (2 * (j % 2) + dy + h) % NZ


class Half(NamedTuple):
    t2: Any
    t1: Any
    p2: Any
    p1: Any
    x2: Any
    x1: Any
    accg: Any
    accu: Any
    hid: Any
    hidp: Any
    part2: Any
    mate2: Any
    part1: Any
    mate1: Any
    far_s: Any
    far_r: Any
    near_s: Any
    near_r: Any
    fin2: Any
    fin1: Any
    r2: Any
    r1: Any
    o2s: Any
    o1s: Any
    o2r: Any
    o1r: Any
    w2hi: Any
    w2lo: Any


def half_scratch(h):
    r, d = RING[h], DIRECT[h]
    bf = lambda *shape: pltpu.VMEM(shape, BF16)
    f = lambda *shape: pltpu.VMEM(shape, F32)
    return Half(
        t2=bf(8, 16, r), t1=bf(8, 16, d), p2=bf(8, 32, r), p1=bf(8, 32, d),
        x2=bf(8, 8, 32, r), x1=bf(2, 8, 32, d),
        accg=f(256, 512), accu=f(256, 512), hid=bf(256, 512), hidp=bf(256, 512),
        part2=bf(2, 4, 4, 64, r), mate2=bf(4, 4, 64, r), part1=bf(2, 8, 32, d), mate1=bf(8, 32, d),
        far_s=bf(2, 4, 32, r), far_r=bf(2, 4, 32, r), near_s=bf(2, 2, 4, 32, r), near_r=bf(2, 2, 4, 32, r),
        fin2=bf(4, 8, 8, r), fin1=bf(8, 32, d), r2=bf(4, 8, 8, r), r1=bf(8, 32, d),
        o2s=bf(2, 4, 16, r), o1s=bf(8, 16, d), o2r=bf(4, 16, r), o1r=bf(8, 16, d),
        w2hi=bf(32, 64), w2lo=bf(32, 64),
    )


def kernel(
    tok_hbm, routes_hbm, combine_hbm, wg_hbm, wu_hbm, wd_hbm, out_ref,
    tok_ref, routes_ref, combine_ref, info_ref, infos, wg, wu, wd, sel, whi, wlo, tally, expert_of, slot_of, before, perm, wrows, wcols, total_ref,
    w_sem, send_sems, recv_sems, *halves,
):
    half = [Half(*halves[:len(Half._fields)]), Half(*halves[len(Half._fields):])]
    ep = lax.axis_index("ep")
    tp = lax.axis_index("tp")
    y, z = ep // NZ, ep % NZ
    x, c = tp // 2, tp % 2
    recv_of = {}
    sent = [0, 0, 0, 0]

    def on_tp(other):
        return {"ep": ep, "tp": other}

    def on_ep(other):
        return {"ep": other, "tp": tp}

    def recv_sem(name):
        return recv_sems.at[recv_of.setdefault(name, len(recv_of))]

    def remote(group, name, src, dst, device):
        size = src.dtype.itemsize
        for dim in src.shape:
            size *= dim
        sent[group] += size // 4096
        pltpu.make_async_remote_copy(
            src_ref=src, dst_ref=dst, send_sem=send_sems.at[group], recv_sem=recv_sem(name),
            device_id=device, device_id_type=MESH,
        ).start()

    def arrived(name, like):
        pltpu.make_async_remote_copy(
            src_ref=like, dst_ref=like, send_sem=send_sems.at[0], recv_sem=recv_sem(name),
            device_id=on_tp(mate), device_id_type=MESH,
        ).wait_recv()

    mate = x * 2 + (1 - c)
    right = ((x + 1) % NX) * 2 + c
    left = ((x + 3) % NX) * 2 + c
    far = ((x + 2) % NX) * 2 + c

    small = []
    for n, (src, dst) in enumerate(
        ((routes_hbm, routes_ref), (combine_hbm, combine_ref), (tok_hbm, tok_ref))
    ):
        load = pltpu.make_async_copy(src, dst, w_sem.at[3 + n])
        load.start()
        small.append(load)
    barrier = pltpu.get_barrier_semaphore()
    for j in range(1, 8):
        pl.semaphore_signal(barrier, inc=1, device_id=on_tp((tp + j) % 8), device_id_type=MESH)
    for dy in range(NY):
        for dz in range(NZ):
            if dy or dz:
                other = ((y + dy) % NY) * NZ + (z + dz) % NZ
                pl.semaphore_signal(barrier, inc=1, device_id=on_ep(other), device_id_type=MESH)
    small[0].wait()
    small[1].wait()
    info_ref[0:2, :] = jnp.concatenate([routes_ref[...].astype(F32)] * 8, axis=1)
    info_ref[2:4, :] = jnp.concatenate([combine_ref[...]] * 8, axis=1)
    info_ref[4:8, :] = jnp.zeros((4, 128), F32)
    small[2].wait()
    pl.semaphore_wait(barrier, 22)

    def ring_cols(h, t):
        return pl.ds(pl.multiple_of(t * RING[h], 128), RING[h])

    def direct_cols(h, core):
        return pl.ds(pl.multiple_of(8 * RING[h] + core * DIRECT[h], 128), DIRECT[h])

    peers = [(tp + j) % 8 for j in (4, 5, 3, 2, 6, 7, 1)]
    for t in peers:
        remote(0, "info", info_ref, infos.at[tp], on_tp(t))
    for h in (A, B):
        for t in peers:
            remote(0, ("t2", h), tok_ref.at[:, ring_cols(h, t)], half[h].t2.at[tp], on_tp(t))
    infos[tp] = info_ref[...]
    for h in (A, B):
        half[h].t2[tp] = tok_ref[:, ring_cols(h, tp)]
        half[h].t1[tp] = tok_ref[:, direct_cols(h, c)]
    loads = []
    for n, (src, dst) in enumerate(((wg_hbm, wg), (wu_hbm, wu), (wd_hbm, wd))):
        load = pltpu.make_async_copy(src, dst, w_sem.at[n])
        load.start()
        loads.append(load)
    row = lax.broadcasted_iota(jnp.int32, (512, 128), 0)
    lane = lax.broadcasted_iota(jnp.int32, (512, 128), 1)
    j_of = (row // 32) % 8
    dy_of = j_of // 2
    dz_of = (2 * (j_of % 2) + dy_of + row // 256) % NZ
    expert_of[...] = (((y + dy_of) % NY) * NZ + (z + dz_of) % NZ).astype(F32)
    same = (lane // 16) == ((row % 32) // 4)
    slot_of[...] = jnp.where(same, row % 4, 128).astype(F32)
    urow = lax.broadcasted_iota(jnp.int32, (128, 128), 0)
    ulane = lax.broadcasted_iota(jnp.int32, (128, 128), 1)
    total_ref[...] = jnp.zeros((16, 4096), F32)
    to = lax.broadcasted_iota(jnp.int32, (256, 256), 0)
    come = lax.broadcasted_iota(jnp.int32, (256, 256), 1)
    home = (x + to // 64) % NX
    perm[...] = jnp.where(come == ((to % 64) // 8) * 32 + home * 8 + to % 8, 1.0, 0.0).astype(BF16)
    before[...] = jnp.where((urow < ulane) & ((urow // 16) == (ulane // 16)), 1.0, 0.0).astype(BF16)
    arrived("info", infos.at[pl.ds(0, 7)])
    for h in (A, B):
        for t in peers:
            remote(0, ("t1", h), tok_ref.at[:, direct_cols(h, t % 2)], half[h].t1.at[tp], on_tp(t))

    lane8 = lax.broadcasted_iota(jnp.int32, (8, 128), 1) // 16
    info = jnp.zeros((8, 128), F32)
    for b in range(8):
        info = info + jnp.where(lane8 == b, infos[b], 0.0)
    expert = expert_of[...]
    first_of = jnp.where(info[0:1] == expert, 1.0, 0.0)
    second_of = jnp.where(info[1:2] == expert, 1.0, 0.0)
    named = first_of + second_of
    count = jnp.dot(named.astype(BF16), before[...], preferred_element_type=F32)
    hit = count == slot_of[...]
    sel[...] = jnp.where(hit, named, 0.0).astype(BF16)

    def pick(h, tokens, width, picked, landing, name):
        rows = sel[h * 256:(h + 1) * 256]
        got = jnp.dot(rows, tokens[...].reshape(128, width), preferred_element_type=F32)
        picked[...] = got.astype(BF16).reshape(8, 32, width)
        order = (4, 5, 6, 7, 2, 3, 1, 0) if h == A else (4, 5, 6, 2, 3, 7, 0, 1)
        for j in order:
            dy, dz = hop(h, j)
            if dy or dz:
                other = ((y + dy) % NY) * NZ + (z + dz) % NZ
                remote(0, (name, h), picked.at[j], landing.at[j], on_ep(other))
            else:
                landing[j] = picked[j]

    def others(h):
        return pl.ds(0, 7 if h == A else 8)

    def pick_ring(h):
        arrived(("t2", h), half[h].t2.at[pl.ds(0, 7)])
        pick(h, half[h].t2, RING[h], half[h].p2, half[h].x2.at[tp], "spread2")

    def pick_direct(h):
        arrived(("t1", h), half[h].t1.at[pl.ds(0, 7)])
        pick(h, half[h].t1, DIRECT[h], half[h].p1, half[h].x1.at[c], "spread1")

    pick_ring(A)
    pick_ring(B)
    weight = jnp.where(hit, first_of * info[2:3] + second_of * info[3:4], 0.0)
    wrows[...] = weight.reshape(16, 32, 128)
    weight = weight.T
    high = weight.astype(BF16)
    whi[...] = high
    wlo[...] = (weight - high.astype(F32)).astype(BF16)
    wcols[...] = wrows[:, pl.ds(pl.multiple_of(x * 8, 8), 8), :].reshape(128, 128).T
    mine = wcols[pl.ds(pl.multiple_of(x * 32, 32), 32), :]
    for h in (A, B):
        part = mine[:, h * 64:(h + 1) * 64]
        high = part.astype(BF16)
        half[h].w2hi[...] = high
        half[h].w2lo[...] = (part - high.astype(F32)).astype(BF16)

    LO, HI, ALL = pl.ds(0, 4), pl.ds(4, 4), pl.ds(0, 8)

    def push(name, t, h, rows, device):
        block = half[h].x2.at[t, rows]
        remote(1, (name, h), block, block, on_tp(device))

    def got(name, h, rows):
        arrived((name, h), half[h].x2.at[0, rows])

    def own_first(h):
        push("m_own", tp, h, ALL, mate)
        push("r_lo", tp, h, LO, right)
        push("l_hi", tp, h, HI, left)

    def own_second(h):
        push("r_hi", tp, h, HI, right)
        push("l_lo", tp, h, LO, left)

    def forward(h):
        got("r_lo", h, LO)
        push("m_left", left, h, LO, mate)
        push("f_lo", left, h, LO, right)
        got("l_hi", h, HI)
        push("m_right", right, h, HI, mate)
        push("f_hi", right, h, HI, left)

    def near_rest(h):
        got("r_hi", h, HI)
        push("m_left", left, h, HI, mate)
        got("l_lo", h, LO)
        push("m_right", right, h, LO, mate)

    def far_rest(h):
        got("f_lo", h, LO)
        push("m_far", far, h, LO, mate)
        got("f_hi", h, HI)
        push("m_far", far, h, HI, mate)

    def direct_share(h):
        x1 = half[h].x1
        arrived(("spread1", h), x1.at[0, others(h)])
        remote(1, ("m_direct", h), x1.at[c], x1.at[c], on_tp(mate))

    def accumulate(h, a, rows, fresh):
        gate = jnp.dot(a, wg[rows, :], preferred_element_type=F32)
        up = jnp.dot(a, wu[rows, :], preferred_element_type=F32)
        if fresh:
            half[h].accg[...] = gate
            half[h].accu[...] = up
        else:
            half[h].accg[...] += gate
            half[h].accu[...] += up

    def gate_up(h, k, name):
        got(name, h, ALL)
        chip = (x + k) % NX
        x2, r = half[h].x2, RING[h]
        a = jnp.concatenate([x2[chip * 2].reshape(256, r), x2[chip * 2 + 1].reshape(256, r)], axis=1)
        accumulate(h, a, pl.ds(pl.multiple_of(chip * 2 * r, 256), 2 * r), k == 0)

    def gate_up_part(h, k, core, name):
        if name is not None:
            got(name, h, ALL)
        t = ((x + k) % NX) * 2 + core
        r = RING[h]
        accumulate(h, half[h].x2[t].reshape(256, r), ring_cols(h, t), False)

    def gate_up_direct_own(h):
        accumulate(h, half[h].x1[c].reshape(256, DIRECT[h]), direct_cols(h, c), False)

    def gate_up_direct_mate(h):
        arrived(("m_direct", h), half[h].x1.at[0])
        accumulate(h, half[h].x1[1 - c].reshape(256, DIRECT[h]), direct_cols(h, 1 - c), False)

    def silu(h):
        gate = half[h].accg[...]
        half[h].hid[...] = (gate / (1.0 + jnp.exp(-gate)) * half[h].accu[...]).astype(BF16)
        half[h].hidp[...] = jnp.dot(perm[...], half[h].hid[...], preferred_element_type=F32).astype(BF16)

    def down(h, g):
        s, r = half[h], RING[h]
        parts = []
        for m in (2 * g, 2 * g + 1):
            cols = pl.ds(m * 2 * r, 2 * r)
            parts.append(jnp.dot(s.hidp[...], wd[:, cols], preferred_element_type=F32).astype(BF16))
        for m, part in zip((2 * g, 2 * g + 1), parts):
            for core in range(2):
                s.part2[core, :, m] = part[:, core * r:(core + 1) * r].reshape(4, 64, r)
        chunks = pl.ds(2 * g, 2)
        remote(2, ("far", h, g), s.part2.at[1 - c, 2, chunks], s.mate2.at[2, chunks], on_tp(mate))
        if g:
            for k in (1, 3, 0):
                remote(2, ("pair", h, k), s.part2.at[1 - c, k], s.mate2.at[k], on_tp(mate))

    def down_direct(h):
        s, d = half[h], DIRECT[h]
        for core in range(2):
            cols = pl.ds(8 * RING[h] + core * d, d)
            part = jnp.dot(s.hid[...], wd[:, cols], preferred_element_type=F32).astype(BF16)
            s.part1[core] = part.reshape(8, 32, d)
        remote(2, ("pair_direct", h), s.part1.at[1 - c], s.mate1, on_tp(mate))

    def paired(h, k):
        arrived(("pair", h, k), half[h].mate2.at[k])

    def chip_sum(h, k, rows, chunks=slice(None)):
        s = half[h]
        rows = pl.ds(rows * 32, 32)
        return s.part2[c, k, chunks, rows, :].astype(F32) + s.mate2[k, chunks, rows, :].astype(F32)

    def reduce_far(h, g):
        s = half[h]
        chunks = pl.ds(2 * g, 2)
        arrived(("far", h, g), s.mate2.at[2, chunks])
        for rows, name, device in ((0, "far_lo", right), (1, "far_hi", left)):
            s.far_s[rows, chunks] = chip_sum(h, 2, rows, chunks).astype(BF16)
            remote(2, (name, h), s.far_s.at[rows, chunks], s.far_r.at[rows, chunks], on_tp(device))

    def near_send(h, side, rows, value):
        s = half[h]
        s.near_s[side, rows] = value.astype(BF16)
        name = ("near_hi" if rows else "near_lo", h)
        remote(2, name, s.near_s.at[side, rows], s.near_r.at[side, rows], on_tp((right, left)[side]))

    def reduce_near_first(h):
        paired(h, 1)
        near_send(h, 0, 1, chip_sum(h, 1, 1))
        paired(h, 3)
        near_send(h, 1, 0, chip_sum(h, 3, 0))

    def reduce_near_second(h):
        s = half[h]
        arrived(("far_lo", h), s.far_r.at[0])
        near_send(h, 0, 0, chip_sum(h, 1, 0) + s.far_r[0].astype(F32))
        arrived(("far_hi", h), s.far_r.at[1])
        near_send(h, 1, 1, chip_sum(h, 3, 1) + s.far_r[1].astype(F32))

    def give_back(h, blocks, fin, landing, name):
        for j in blocks:
            at = (slice(None), j) if name == "back2" else (j,)
            dy, dz = hop(h, j)
            if dy or dz:
                other = ((y + NY - dy) % NY) * NZ + (z + NZ - dz) % NZ
                remote(3, (name, h), fin.at[at], landing.at[at], on_ep(other))
            else:
                landing[at] = fin[at]

    def reduce_last(h):
        s = half[h]
        paired(h, 0)
        near_r = s.near_r
        for rows, name in ((1, "near_hi"), (0, "near_lo")):
            arrived((name, h), near_r.at[0])
            total = chip_sum(h, 0, rows)
            total = total + near_r[0, rows].astype(F32) + near_r[1, rows].astype(F32)
            s.fin2[:, rows * 4:rows * 4 + 4] = total.reshape(4, 4, 8, RING[h]).astype(BF16)
            give_back(h, range(rows * 4, rows * 4 + 4), s.fin2, s.r2, "back2")

    def direct_back(h):
        s = half[h]
        arrived(("pair_direct", h), s.mate1)
        s.fin1[...] = (s.part1[c].astype(F32) + s.mate1[...].astype(F32)).astype(BF16)
        give_back(h, (4, 5, 6, 7, 2, 3, 0, 1), s.fin1, s.r1, "back1")

    def weigh_ring(h):
        s, r = half[h], RING[h]
        arrived(("back2", h), s.r2.at[:, others(h)])
        for m in range(NX):
            rows = s.r2[m].astype(F32).reshape(64, r).astype(BF16)
            total = jnp.dot(s.w2hi[...], rows, preferred_element_type=F32)
            total = total + jnp.dot(s.w2lo[...], rows, preferred_element_type=F32)
            s.o2s[:, m] = total.astype(BF16).reshape(2, 16, r)
        remote(3, ("out2", h), s.o2s.at[1 - c], s.o2r, on_tp(mate))

    def weigh_direct(h):
        s, d = half[h], DIRECT[h]
        arrived(("back1", h), s.r1.at[others(h)])
        rows = s.r1[...].reshape(256, d)
        cols = slice(h * 256, (h + 1) * 256)
        total = jnp.dot(whi[:, cols], rows, preferred_element_type=F32)
        total = total + jnp.dot(wlo[:, cols], rows, preferred_element_type=F32)
        s.o1s[...] = total.astype(BF16).reshape(8, 16, d)
        for t in peers:
            remote(3, ("out1", h), s.o1s.at[t], s.o1r.at[tp], on_tp(t))
        s.o1r[tp] = s.o1s[tp]

    def put(cols, value):
        total_ref[:, cols] += value

    def finish_direct(h):
        s, d = half[h], DIRECT[h]
        arrived(("out1", h), s.o1r.at[pl.ds(0, 7)])
        for core in range(2):
            piece = s.o1r[core].astype(F32)
            for chip in range(1, NX):
                piece = piece + s.o1r[chip * 2 + core].astype(F32)
            put(pl.ds(8 * RING[h] + core * d, d), piece)

    def finish_ring(h):
        s = half[h]
        arrived(("out2", h), s.o2r)
        for m in range(NX):
            put(ring_cols(h, 2 * m + c), s.o2s[c, m].astype(F32))
            put(ring_cols(h, 2 * m + 1 - c), s.o2r[m].astype(F32))

    arrived(("spread2", A), half[A].x2.at[0, others(A)])
    own_first(A)
    own_second(A)
    pick_direct(A)
    loads[0].wait()
    loads[1].wait()
    gate_up(A, 0, "m_own")
    arrived(("spread2", B), half[B].x2.at[0, others(B)])
    forward(A)
    own_first(B)
    own_second(B)
    pick_direct(B)
    near_rest(A)
    gate_up(A, 3, "m_left")
    gate_up(A, 1, "m_right")
    gate_up(B, 0, "m_own")
    far_rest(A)
    gate_up_part(A, 2, c, None)
    direct_share(A)
    gate_up_direct_own(A)
    gate_up_part(A, 2, 1 - c, "m_far")
    forward(B)
    near_rest(B)
    gate_up_direct_mate(A)
    silu(A)
    loads[2].wait()
    down(A, 0)
    down(A, 1)
    direct_share(B)
    gate_up(B, 3, "m_left")
    reduce_far(A, 0)
    reduce_far(A, 1)
    gate_up(B, 1, "m_right")
    reduce_near_first(A)
    far_rest(B)
    down_direct(A)
    gate_up_direct_own(B)
    gate_up(B, 2, "m_far")
    gate_up_direct_mate(B)
    silu(B)
    down(B, 0)
    reduce_near_second(A)
    direct_back(A)
    down(B, 1)
    reduce_far(B, 0)
    reduce_far(B, 1)
    down_direct(B)
    reduce_near_first(B)
    direct_back(B)
    reduce_last(A)
    reduce_near_second(B)
    reduce_last(B)
    weigh_direct(A)
    weigh_direct(B)
    weigh_ring(A)
    finish_ring(A)
    weigh_ring(B)
    finish_ring(B)
    finish_direct(A)
    finish_direct(B)
    pass
    out_ref[...] = total_ref[...].astype(BF16)
    for group in range(4):
        every = tally.at[pl.ds(0, sent[group])]
        pltpu.make_async_remote_copy(
            src_ref=every, dst_ref=every, send_sem=send_sems.at[group], recv_sem=recv_sems.at[0],
            device_id=on_tp(mate), device_id_type=MESH,
        ).wait_send()
    assert len(recv_of) == RECVS, len(recv_of)


def body(tokens, routes, combine, gate_weight, up_weight, down_weight):
    vmem = pl.BlockSpec(memory_space=pltpu.VMEM)
    hbm = pl.BlockSpec(memory_space=pltpu.HBM)
    dma = pltpu.SemaphoreType.DMA
    return pl.pallas_call(
        kernel,
        out_shape=jax.ShapeDtypeStruct((16, 4096), BF16),
        in_specs=[hbm] * 6,
        out_specs=vmem,
        scratch_shapes=[
            pltpu.VMEM((16, 4096), BF16),
            pltpu.VMEM((2, 16), jnp.int32),
            pltpu.VMEM((2, 16), F32),
            pltpu.VMEM((8, 128), F32),
            pltpu.VMEM((8, 8, 128), F32),
            pltpu.VMEM((4096, 512), BF16),
            pltpu.VMEM((4096, 512), BF16),
            pltpu.VMEM((512, 4096), BF16),
            pltpu.VMEM((512, 128), BF16),
            pltpu.VMEM((128, 512), BF16),
            pltpu.VMEM((128, 512), BF16),
            pltpu.VMEM((TALLY, 8, 128), F32),
            pltpu.VMEM((512, 128), F32),
            pltpu.VMEM((512, 128), F32),
            pltpu.VMEM((128, 128), BF16),
            pltpu.VMEM((256, 256), BF16),
            pltpu.VMEM((16, 32, 128), F32),
            pltpu.VMEM((128, 128), F32),
            pltpu.VMEM((16, 4096), F32),
            dma((6,)),
            dma((4,)),
            dma((RECVS,)),
            *half_scratch(A),
            *half_scratch(B),
        ],
        compiler_params=pltpu.CompilerParams(
            collective_id=0, has_side_effects=True, vmem_limit_bytes=60 * 1024 * 1024
        ),
        name="moe",
    )(tokens, routes.T, combine.T, gate_weight[0], up_weight[0], down_weight[0])


def solution(mesh):
    return jax.shard_map(
        body,
        mesh=mesh,
        in_specs=(
            P(("ep", "tp"), None),
            P(("ep", "tp"), None),
            P(("ep", "tp"), None),
            P("ep", None, "tp"),
            P("ep", None, "tp"),
            P("ep", "tp", None),
        ),
        out_specs=P(("ep", "tp"), None),
        check_vma=False,
    )
```

```python
from typing import Any, NamedTuple

import jax
import jax.numpy as jnp
from jax import lax
from jax.experimental import pallas as pl
from jax.experimental.pallas import tpu as pltpu
from jax.sharding import PartitionSpec as P

MESH = pl.DeviceIdType.MESH
F32 = jnp.float32
BF16 = jnp.bfloat16
NX, NY, NZ = 4, 4, 4
A, B = 0, 1
RING = (256, 384)
DIRECT = (1024, 512)
RECVS = 63
TALLY = 1024


def hop(h, j):
    dy = j // 2
    return dy, (2 * (j % 2) + dy + h) % NZ


class Half(NamedTuple):
    t2: Any
    t1: Any
    p2: Any
    p1: Any
    x2: Any
    x1: Any
    accg: Any
    accu: Any
    hid: Any
    hidp: Any
    part2: Any
    mate2: Any
    part1: Any
    mate1: Any
    far_s: Any
    far_r: Any
    near_s: Any
    near_r: Any
    fin2: Any
    fin1: Any
    r2: Any
    r1: Any
    o2s: Any
    o1s: Any
    o2r: Any
    o1r: Any
    w2hi: Any
    w2lo: Any


def half_scratch(h):
    r, d = RING[h], DIRECT[h]
    bf = lambda *shape: pltpu.VMEM(shape, BF16)
    f = lambda *shape: pltpu.VMEM(shape, F32)
    return Half(
        t2=bf(8, 16, r), t1=bf(8, 16, d), p2=bf(8, 32, r), p1=bf(8, 32, d),
        x2=bf(8, 8, 32, r), x1=bf(2, 8, 32, d),
        accg=f(256, 512), accu=f(256, 512), hid=bf(256, 512), hidp=bf(256, 512),
        part2=bf(2, 4, 4, 64, r), mate2=bf(4, 4, 64, r), part1=bf(2, 8, 32, d), mate1=bf(8, 32, d),
        far_s=bf(2, 4, 32, r), far_r=bf(2, 4, 32, r), near_s=bf(2, 2, 4, 32, r), near_r=bf(2, 2, 4, 32, r),
        fin2=bf(4, 8, 8, r), fin1=bf(8, 32, d), r2=bf(4, 8, 8, r), r1=bf(8, 32, d),
        o2s=bf(2, 4, 16, r), o1s=bf(8, 16, d), o2r=bf(4, 16, r), o1r=bf(8, 16, d),
        w2hi=bf(32, 64), w2lo=bf(32, 64),
    )


def kernel(
    tok_hbm, routes_hbm, combine_hbm, wg_hbm, wu_hbm, wd_hbm, out_ref,
    tok_ref, routes_ref, combine_ref, info_ref, infos, wg, wu, wd, sel, whi, wlo, tally, expert_of, slot_of, before, perm, wrows, wcols, total_ref,
    w_sem, send_sems, recv_sems, *halves,
):
    half = [Half(*halves[:len(Half._fields)]), Half(*halves[len(Half._fields):])]
    ep = lax.axis_index("ep")
    tp = lax.axis_index("tp")
    y, z = ep // NZ, ep % NZ
    x, c = tp // 2, tp % 2
    recv_of = {}
    sent = [0, 0, 0, 0]

    def on_tp(other):
        return {"ep": ep, "tp": other}

    def on_ep(other):
        return {"ep": other, "tp": tp}

    def recv_sem(name):
        return recv_sems.at[recv_of.setdefault(name, len(recv_of))]

    def remote(group, name, src, dst, device):
        size = src.dtype.itemsize
        for dim in src.shape:
            size *= dim
        sent[group] += size // 4096
        pltpu.make_async_remote_copy(
            src_ref=src, dst_ref=dst, send_sem=send_sems.at[group], recv_sem=recv_sem(name),
            device_id=device, device_id_type=MESH,
        ).start()

    def arrived(name, like):
        pltpu.make_async_remote_copy(
            src_ref=like, dst_ref=like, send_sem=send_sems.at[0], recv_sem=recv_sem(name),
            device_id=on_tp(mate), device_id_type=MESH,
        ).wait_recv()

    mate = x * 2 + (1 - c)
    right = ((x + 1) % NX) * 2 + c
    left = ((x + 3) % NX) * 2 + c
    far = ((x + 2) % NX) * 2 + c

    small = []
    for n, (src, dst) in enumerate(
        ((routes_hbm, routes_ref), (combine_hbm, combine_ref), (tok_hbm, tok_ref))
    ):
        load = pltpu.make_async_copy(src, dst, w_sem.at[3 + n])
        load.start()
        small.append(load)
    barrier = pltpu.get_barrier_semaphore()
    for j in range(1, 8):
        pl.semaphore_signal(barrier, inc=1, device_id=on_tp((tp + j) % 8), device_id_type=MESH)
    for dy in range(NY):
        for dz in range(NZ):
            if dy or dz:
                other = ((y + dy) % NY) * NZ + (z + dz) % NZ
                pl.semaphore_signal(barrier, inc=1, device_id=on_ep(other), device_id_type=MESH)
    small[0].wait()
    small[1].wait()
    info_ref[0:2, :] = jnp.concatenate([routes_ref[...].astype(F32)] * 8, axis=1)
    info_ref[2:4, :] = jnp.concatenate([combine_ref[...]] * 8, axis=1)
    info_ref[4:8, :] = jnp.zeros((4, 128), F32)
    small[2].wait()
    pl.semaphore_wait(barrier, 22)

    def ring_cols(h, t):
        return pl.ds(pl.multiple_of(t * RING[h], 128), RING[h])

    def direct_cols(h, core):
        return pl.ds(pl.multiple_of(8 * RING[h] + core * DIRECT[h], 128), DIRECT[h])

    peers = [(tp + j) % 8 for j in (4, 5, 3, 2, 6, 7, 1)]
    for t in peers:
        remote(0, "info", info_ref, infos.at[tp], on_tp(t))
    for h in (A, B):
        for t in peers:
            remote(0, ("t2", h), tok_ref.at[:, ring_cols(h, t)], half[h].t2.at[tp], on_tp(t))
    for t in peers:
        remote(0, ("t1", A), tok_ref.at[:, direct_cols(A, t % 2)], half[A].t1.at[tp], on_tp(t))
    infos[tp] = info_ref[...]
    for h in (A, B):
        half[h].t2[tp] = tok_ref[:, ring_cols(h, tp)]
        half[h].t1[tp] = tok_ref[:, direct_cols(h, c)]
    loads = []
    for n, (src, dst) in enumerate(((wg_hbm, wg), (wu_hbm, wu), (wd_hbm, wd))):
        load = pltpu.make_async_copy(src, dst, w_sem.at[n])
        load.start()
        loads.append(load)
    row = lax.broadcasted_iota(jnp.int32, (512, 128), 0)
    lane = lax.broadcasted_iota(jnp.int32, (512, 128), 1)
    j_of = (row // 32) % 8
    dy_of = j_of // 2
    dz_of = (2 * (j_of % 2) + dy_of + row // 256) % NZ
    expert_of[...] = (((y + dy_of) % NY) * NZ + (z + dz_of) % NZ).astype(F32)
    same = (lane // 16) == ((row % 32) // 4)
    slot_of[...] = jnp.where(same, row % 4, 128).astype(F32)
    urow = lax.broadcasted_iota(jnp.int32, (128, 128), 0)
    ulane = lax.broadcasted_iota(jnp.int32, (128, 128), 1)
    total_ref[...] = jnp.zeros((16, 4096), F32)
    to = lax.broadcasted_iota(jnp.int32, (256, 256), 0)
    come = lax.broadcasted_iota(jnp.int32, (256, 256), 1)
    home = (x + to // 64) % NX
    perm[...] = jnp.where(come == ((to % 64) // 8) * 32 + home * 8 + to % 8, 1.0, 0.0).astype(BF16)
    before[...] = jnp.where((urow < ulane) & ((urow // 16) == (ulane // 16)), 1.0, 0.0).astype(BF16)
    arrived("info", infos.at[pl.ds(0, 7)])
    for t in peers:
        remote(0, ("t1", B), tok_ref.at[:, direct_cols(B, t % 2)], half[B].t1.at[tp], on_tp(t))

    lane8 = lax.broadcasted_iota(jnp.int32, (8, 128), 1) // 16
    info = jnp.zeros((8, 128), F32)
    for b in range(8):
        info = info + jnp.where(lane8 == b, infos[b], 0.0)
    expert = expert_of[...]
    first_of = jnp.where(info[0:1] == expert, 1.0, 0.0)
    second_of = jnp.where(info[1:2] == expert, 1.0, 0.0)
    named = first_of + second_of
    count = jnp.dot(named.astype(BF16), before[...], preferred_element_type=F32)
    hit = count == slot_of[...]
    sel[...] = jnp.where(hit, named, 0.0).astype(BF16)

    def pick(h, tokens, width, picked, landing, name):
        rows = sel[h * 256:(h + 1) * 256]
        got = jnp.dot(rows, tokens[...].reshape(128, width), preferred_element_type=F32)
        picked[...] = got.astype(BF16).reshape(8, 32, width)
        order = (4, 5, 6, 7, 2, 3, 1, 0) if h == A else (4, 5, 6, 2, 3, 7, 0, 1)
        for j in order:
            dy, dz = hop(h, j)
            if dy or dz:
                other = ((y + dy) % NY) * NZ + (z + dz) % NZ
                remote(0, (name, h), picked.at[j], landing.at[j], on_ep(other))
            else:
                landing[j] = picked[j]

    def others(h):
        return pl.ds(0, 7 if h == A else 8)

    def pick_ring(h):
        arrived(("t2", h), half[h].t2.at[pl.ds(0, 7)])
        pick(h, half[h].t2, RING[h], half[h].p2, half[h].x2.at[tp], "spread2")

    def pick_direct(h):
        arrived(("t1", h), half[h].t1.at[pl.ds(0, 7)])
        pick(h, half[h].t1, DIRECT[h], half[h].p1, half[h].x1.at[c], "spread1")

    pick_ring(A)
    pick_ring(B)
    weight = jnp.where(hit, first_of * info[2:3] + second_of * info[3:4], 0.0)
    wrows[...] = weight.reshape(16, 32, 128)
    weight = weight.T
    high = weight.astype(BF16)
    whi[...] = high
    wlo[...] = (weight - high.astype(F32)).astype(BF16)
    wcols[...] = wrows[:, pl.ds(pl.multiple_of(x * 8, 8), 8), :].reshape(128, 128).T
    mine = wcols[pl.ds(pl.multiple_of(x * 32, 32), 32), :]
    for h in (A, B):
        part = mine[:, h * 64:(h + 1) * 64]
        high = part.astype(BF16)
        half[h].w2hi[...] = high
        half[h].w2lo[...] = (part - high.astype(F32)).astype(BF16)

    LO, HI, ALL = pl.ds(0, 4), pl.ds(4, 4), pl.ds(0, 8)

    def push(name, t, h, rows, device):
        block = half[h].x2.at[t, rows]
        remote(1, (name, h), block, block, on_tp(device))

    def got(name, h, rows):
        arrived((name, h), half[h].x2.at[0, rows])

    def own_first(h):
        push("m_own", tp, h, ALL, mate)
        push("r_lo", tp, h, LO, right)
        push("l_hi", tp, h, HI, left)

    def own_second(h):
        push("r_hi", tp, h, HI, right)
        push("l_lo", tp, h, LO, left)

    def forward(h):
        got("r_lo", h, LO)
        push("m_left", left, h, LO, mate)
        push("f_lo", left, h, LO, right)
        got("l_hi", h, HI)
        push("m_right", right, h, HI, mate)
        push("f_hi", right, h, HI, left)

    def near_rest(h):
        got("r_hi", h, HI)
        push("m_left", left, h, HI, mate)
        got("l_lo", h, LO)
        push("m_right", right, h, LO, mate)

    def far_rest(h):
        got("f_lo", h, LO)
        push("m_far", far, h, LO, mate)
        got("f_hi", h, HI)
        push("m_far", far, h, HI, mate)

    def direct_share(h):
        x1 = half[h].x1
        arrived(("spread1", h), x1.at[0, others(h)])
        remote(1, ("m_direct", h), x1.at[c], x1.at[c], on_tp(mate))

    def accumulate(h, a, rows, fresh):
        gate = jnp.dot(a, wg[rows, :], preferred_element_type=F32)
        up = jnp.dot(a, wu[rows, :], preferred_element_type=F32)
        if fresh:
            half[h].accg[...] = gate
            half[h].accu[...] = up
        else:
            half[h].accg[...] += gate
            half[h].accu[...] += up

    def gate_up(h, k, name):
        got(name, h, ALL)
        chip = (x + k) % NX
        x2, r = half[h].x2, RING[h]
        a = jnp.concatenate([x2[chip * 2].reshape(256, r), x2[chip * 2 + 1].reshape(256, r)], axis=1)
        accumulate(h, a, pl.ds(pl.multiple_of(chip * 2 * r, 256), 2 * r), k == 0)

    def gate_up_part(h, k, core, name):
        if name is not None:
            got(name, h, ALL)
        t = ((x + k) % NX) * 2 + core
        r = RING[h]
        accumulate(h, half[h].x2[t].reshape(256, r), ring_cols(h, t), False)

    def gate_up_direct_own(h):
        accumulate(h, half[h].x1[c].reshape(256, DIRECT[h]), direct_cols(h, c), False)

    def gate_up_direct_mate(h):
        arrived(("m_direct", h), half[h].x1.at[0])
        accumulate(h, half[h].x1[1 - c].reshape(256, DIRECT[h]), direct_cols(h, 1 - c), False)

    def silu(h):
        gate = half[h].accg[...]
        half[h].hid[...] = (gate / (1.0 + jnp.exp(-gate)) * half[h].accu[...]).astype(BF16)
        half[h].hidp[...] = jnp.dot(perm[...], half[h].hid[...], preferred_element_type=F32).astype(BF16)

    def down(h, g):
        s, r = half[h], RING[h]
        parts = []
        for m in (2 * g, 2 * g + 1):
            cols = pl.ds(m * 2 * r, 2 * r)
            parts.append(jnp.dot(s.hidp[...], wd[:, cols], preferred_element_type=F32).astype(BF16))
        for m, part in zip((2 * g, 2 * g + 1), parts):
            for core in range(2):
                s.part2[core, :, m] = part[:, core * r:(core + 1) * r].reshape(4, 64, r)
        chunks = pl.ds(2 * g, 2)
        remote(2, ("far", h, g), s.part2.at[1 - c, 2, chunks], s.mate2.at[2, chunks], on_tp(mate))
        if g:
            for k in (1, 3, 0):
                remote(2, ("pair", h, k), s.part2.at[1 - c, k], s.mate2.at[k], on_tp(mate))

    def down_direct(h):
        s, d = half[h], DIRECT[h]
        for core in range(2):
            cols = pl.ds(8 * RING[h] + core * d, d)
            part = jnp.dot(s.hid[...], wd[:, cols], preferred_element_type=F32).astype(BF16)
            s.part1[core] = part.reshape(8, 32, d)
        remote(2, ("pair_direct", h), s.part1.at[1 - c], s.mate1, on_tp(mate))

    def paired(h, k):
        arrived(("pair", h, k), half[h].mate2.at[k])

    def chip_sum(h, k, rows, chunks=slice(None)):
        s = half[h]
        rows = pl.ds(rows * 32, 32)
        return s.part2[c, k, chunks, rows, :].astype(F32) + s.mate2[k, chunks, rows, :].astype(F32)

    def reduce_far(h, g):
        s = half[h]
        chunks = pl.ds(2 * g, 2)
        arrived(("far", h, g), s.mate2.at[2, chunks])
        for rows, name, device in ((0, "far_lo", right), (1, "far_hi", left)):
            s.far_s[rows, chunks] = chip_sum(h, 2, rows, chunks).astype(BF16)
            remote(2, (name, h, g), s.far_s.at[rows, chunks], s.far_r.at[rows, chunks], on_tp(device))

    def near_send(h, side, rows, value, chunks=pl.ds(0, 4)):
        s = half[h]
        s.near_s[side, rows, chunks] = value.astype(BF16)
        name = ("near_hi" if rows else "near_lo", h)
        at = (side, rows, chunks)
        remote(2, name, s.near_s.at[at], s.near_r.at[at], on_tp((right, left)[side]))

    def reduce_near_first(h):
        paired(h, 1)
        near_send(h, 0, 1, chip_sum(h, 1, 1))
        paired(h, 3)
        near_send(h, 1, 0, chip_sum(h, 3, 0))

    def reduce_near_second(h, g):
        s = half[h]
        chunks = pl.ds(2 * g, 2)
        arrived(("far_lo", h, g), s.far_r.at[0, chunks])
        near_send(h, 0, 0, chip_sum(h, 1, 0, chunks) + s.far_r[0, chunks].astype(F32), chunks)
        arrived(("far_hi", h, g), s.far_r.at[1, chunks])
        near_send(h, 1, 1, chip_sum(h, 3, 1, chunks) + s.far_r[1, chunks].astype(F32), chunks)

    def give_back(h, blocks, fin, landing, name):
        for j in blocks:
            at = (slice(None), j) if name == "back2" else (j,)
            dy, dz = hop(h, j)
            if dy or dz:
                other = ((y + NY - dy) % NY) * NZ + (z + NZ - dz) % NZ
                remote(3, (name, h), fin.at[at], landing.at[at], on_ep(other))
            else:
                landing[at] = fin[at]

    def reduce_last(h):
        s = half[h]
        paired(h, 0)
        near_r = s.near_r
        for rows, name in ((1, "near_hi"), (0, "near_lo")):
            arrived((name, h), near_r.at[0])
            total = chip_sum(h, 0, rows)
            total = total + near_r[0, rows].astype(F32) + near_r[1, rows].astype(F32)
            s.fin2[:, rows * 4:rows * 4 + 4] = total.reshape(4, 4, 8, RING[h]).astype(BF16)
            give_back(h, range(rows * 4, rows * 4 + 4), s.fin2, s.r2, "back2")

    def direct_back(h):
        s = half[h]
        arrived(("pair_direct", h), s.mate1)
        s.fin1[...] = (s.part1[c].astype(F32) + s.mate1[...].astype(F32)).astype(BF16)
        give_back(h, (4, 5, 6, 7, 2, 3, 0, 1), s.fin1, s.r1, "back1")

    def weigh_ring(h):
        s, r = half[h], RING[h]
        arrived(("back2", h), s.r2.at[:, others(h)])
        for m in range(NX):
            rows = s.r2[m].astype(F32).reshape(64, r).astype(BF16)
            total = jnp.dot(s.w2hi[...], rows, preferred_element_type=F32)
            total = total + jnp.dot(s.w2lo[...], rows, preferred_element_type=F32)
            s.o2s[:, m] = total.astype(BF16).reshape(2, 16, r)
        remote(3, ("out2", h), s.o2s.at[1 - c], s.o2r, on_tp(mate))

    def weigh_direct(h):
        s, d = half[h], DIRECT[h]
        arrived(("back1", h), s.r1.at[others(h)])
        rows = s.r1[...].reshape(256, d)
        cols = slice(h * 256, (h + 1) * 256)
        total = jnp.dot(whi[:, cols], rows, preferred_element_type=F32)
        total = total + jnp.dot(wlo[:, cols], rows, preferred_element_type=F32)
        s.o1s[...] = total.astype(BF16).reshape(8, 16, d)
        for t in peers:
            remote(3, ("out1", h), s.o1s.at[t], s.o1r.at[tp], on_tp(t))
        s.o1r[tp] = s.o1s[tp]

    def put(cols, value):
        total_ref[:, cols] += value

    def finish_direct(h):
        s, d = half[h], DIRECT[h]
        arrived(("out1", h), s.o1r.at[pl.ds(0, 7)])
        for core in range(2):
            piece = s.o1r[core].astype(F32)
            for chip in range(1, NX):
                piece = piece + s.o1r[chip * 2 + core].astype(F32)
            put(pl.ds(8 * RING[h] + core * d, d), piece)

    def finish_ring(h):
        s = half[h]
        arrived(("out2", h), s.o2r)
        for m in range(NX):
            put(ring_cols(h, 2 * m + c), s.o2s[c, m].astype(F32))
            put(ring_cols(h, 2 * m + 1 - c), s.o2r[m].astype(F32))

    pick_direct(A)
    arrived(("spread2", A), half[A].x2.at[0, others(A)])
    own_first(A)
    own_second(A)
    loads[0].wait()
    loads[1].wait()
    gate_up(A, 0, "m_own")
    arrived(("spread2", B), half[B].x2.at[0, others(B)])
    forward(A)
    own_first(B)
    own_second(B)
    pick_direct(B)
    near_rest(A)
    gate_up(A, 3, "m_left")
    gate_up(A, 1, "m_right")
    gate_up(B, 0, "m_own")
    far_rest(A)
    direct_share(A)
    gate_up_part(A, 2, c, None)
    gate_up_direct_own(A)
    gate_up_part(A, 2, 1 - c, "m_far")
    forward(B)
    gate_up_direct_mate(A)
    direct_share(B)
    silu(A)
    loads[2].wait()
    down(A, 0)
    down(A, 1)
    near_rest(B)
    down_direct(A)
    reduce_far(A, 0)
    reduce_far(A, 1)
    gate_up_direct_own(B)
    gate_up_direct_mate(B)
    far_rest(B)
    reduce_near_first(A)
    gate_up(B, 3, "m_left")
    gate_up(B, 1, "m_right")
    direct_back(A)
    gate_up_part(B, 2, c, None)
    gate_up_part(B, 2, 1 - c, "m_far")
    silu(B)
    down(B, 0)
    reduce_near_second(A, 0)
    reduce_near_second(A, 1)
    down(B, 1)
    reduce_far(B, 0)
    reduce_far(B, 1)
    reduce_near_first(B)
    down_direct(B)
    direct_back(B)
    reduce_last(A)
    reduce_near_second(B, 0)
    reduce_near_second(B, 1)
    reduce_last(B)
    weigh_direct(A)
    weigh_direct(B)
    weigh_ring(A)
    weigh_ring(B)
    finish_ring(A)
    finish_ring(B)
    finish_direct(A)
    finish_direct(B)
    pass
    out_ref[...] = total_ref[...].astype(BF16)
    for group in range(4):
        every = tally.at[pl.ds(0, sent[group])]
        pltpu.make_async_remote_copy(
            src_ref=every, dst_ref=every, send_sem=send_sems.at[group], recv_sem=recv_sems.at[0],
            device_id=on_tp(mate), device_id_type=MESH,
        ).wait_send()
    assert len(recv_of) == RECVS, len(recv_of)


def body(tokens, routes, combine, gate_weight, up_weight, down_weight):
    vmem = pl.BlockSpec(memory_space=pltpu.VMEM)
    hbm = pl.BlockSpec(memory_space=pltpu.HBM)
    dma = pltpu.SemaphoreType.DMA
    return pl.pallas_call(
        kernel,
        out_shape=jax.ShapeDtypeStruct((16, 4096), BF16),
        in_specs=[hbm] * 6,
        out_specs=vmem,
        scratch_shapes=[
            pltpu.VMEM((16, 4096), BF16),
            pltpu.VMEM((2, 16), jnp.int32),
            pltpu.VMEM((2, 16), F32),
            pltpu.VMEM((8, 128), F32),
            pltpu.VMEM((8, 8, 128), F32),
            pltpu.VMEM((4096, 512), BF16),
            pltpu.VMEM((4096, 512), BF16),
            pltpu.VMEM((512, 4096), BF16),
            pltpu.VMEM((512, 128), BF16),
            pltpu.VMEM((128, 512), BF16),
            pltpu.VMEM((128, 512), BF16),
            pltpu.VMEM((TALLY, 8, 128), F32),
            pltpu.VMEM((512, 128), F32),
            pltpu.VMEM((512, 128), F32),
            pltpu.VMEM((128, 128), BF16),
            pltpu.VMEM((256, 256), BF16),
            pltpu.VMEM((16, 32, 128), F32),
            pltpu.VMEM((128, 128), F32),
            pltpu.VMEM((16, 4096), F32),
            dma((6,)),
            dma((4,)),
            dma((RECVS,)),
            *half_scratch(A),
            *half_scratch(B),
        ],
        compiler_params=pltpu.CompilerParams(
            collective_id=0, has_side_effects=True, vmem_limit_bytes=60 * 1024 * 1024
        ),
        name="moe",
    )(tokens, routes.T, combine.T, gate_weight[0], up_weight[0], down_weight[0])


def solution(mesh):
    return jax.shard_map(
        body,
        mesh=mesh,
        in_specs=(
            P(("ep", "tp"), None),
            P(("ep", "tp"), None),
            P(("ep", "tp"), None),
            P("ep", None, "tp"),
            P("ep", None, "tp"),
            P("ep", "tp", None),
        ),
        out_specs=P(("ep", "tp"), None),
        check_vma=False,
    )
```

```python
from typing import Any, NamedTuple

import jax
import jax.numpy as jnp
from jax import lax
from jax.experimental import pallas as pl
from jax.experimental.pallas import tpu as pltpu
from jax.sharding import PartitionSpec as P

MESH = pl.DeviceIdType.MESH
F32 = jnp.float32
BF16 = jnp.bfloat16
NX, NY, NZ = 4, 4, 4
A, B = 0, 1
RING = (256, 384)
DIRECT = (1024, 512)
RECVS = 63
TALLY = 1024


def hop(h, j):
    dy = j // 2
    return dy, (2 * (j % 2) + dy + h) % NZ


class Half(NamedTuple):
    t2: Any
    t1: Any
    p2: Any
    p1: Any
    x2: Any
    x1: Any
    accg: Any
    accu: Any
    hid: Any
    hidp: Any
    part2: Any
    mate2: Any
    part1: Any
    mate1: Any
    far_s: Any
    far_r: Any
    near_s: Any
    near_r: Any
    fin2: Any
    fin1: Any
    r2: Any
    r1: Any
    o2s: Any
    o1s: Any
    o2r: Any
    o1r: Any
    w2hi: Any
    w2lo: Any


def half_scratch(h):
    r, d = RING[h], DIRECT[h]
    bf = lambda *shape: pltpu.VMEM(shape, BF16)
    f = lambda *shape: pltpu.VMEM(shape, F32)
    return Half(
        t2=bf(8, 16, r), t1=bf(8, 16, d), p2=bf(8, 32, r), p1=bf(8, 32, d),
        x2=bf(8, 8, 32, r), x1=bf(2, 8, 32, d),
        accg=f(256, 512), accu=f(256, 512), hid=bf(256, 512), hidp=bf(256, 512),
        part2=bf(2, 4, 4, 64, r), mate2=bf(4, 4, 64, r), part1=bf(2, 8, 32, d), mate1=bf(8, 32, d),
        far_s=bf(2, 4, 32, r), far_r=bf(2, 4, 32, r), near_s=bf(2, 2, 4, 32, r), near_r=bf(2, 2, 4, 32, r),
        fin2=bf(4, 8, 8, r), fin1=bf(8, 32, d), r2=bf(4, 8, 8, r), r1=bf(8, 32, d),
        o2s=bf(2, 4, 16, r), o1s=bf(8, 16, d), o2r=bf(4, 16, r), o1r=bf(8, 16, d),
        w2hi=bf(32, 64), w2lo=bf(32, 64),
    )


def kernel(
    tok_hbm, routes_hbm, combine_hbm, wg_hbm, wu_hbm, wd_hbm, out_ref,
    tok_ref, routes_ref, combine_ref, info_ref, infos, wg, wu, wd, sel, whi, wlo, tally, expert_of, slot_of, before, perm, wrows, wcols, total_ref,
    w_sem, send_sems, recv_sems, *halves,
):
    half = [Half(*halves[:len(Half._fields)]), Half(*halves[len(Half._fields):])]
    ep = lax.axis_index("ep")
    tp = lax.axis_index("tp")
    y, z = ep // NZ, ep % NZ
    x, c = tp // 2, tp % 2
    recv_of = {}
    sent = [0, 0, 0, 0]

    def on_tp(other):
        return {"ep": ep, "tp": other}

    def on_ep(other):
        return {"ep": other, "tp": tp}

    def recv_sem(name):
        return recv_sems.at[recv_of.setdefault(name, len(recv_of))]

    def remote(group, name, src, dst, device):
        size = src.dtype.itemsize
        for dim in src.shape:
            size *= dim
        sent[group] += size // 4096
        pltpu.make_async_remote_copy(
            src_ref=src, dst_ref=dst, send_sem=send_sems.at[group], recv_sem=recv_sem(name),
            device_id=device, device_id_type=MESH,
        ).start()

    def arrived(name, like):
        pltpu.make_async_remote_copy(
            src_ref=like, dst_ref=like, send_sem=send_sems.at[0], recv_sem=recv_sem(name),
            device_id=on_tp(mate), device_id_type=MESH,
        ).wait_recv()

    mate = x * 2 + (1 - c)
    right = ((x + 1) % NX) * 2 + c
    left = ((x + 3) % NX) * 2 + c
    far = ((x + 2) % NX) * 2 + c

    small = []
    for n, (src, dst) in enumerate(
        ((routes_hbm, routes_ref), (combine_hbm, combine_ref), (tok_hbm, tok_ref))
    ):
        load = pltpu.make_async_copy(src, dst, w_sem.at[3 + n])
        load.start()
        small.append(load)
    barrier = pltpu.get_barrier_semaphore()
    for j in range(1, 8):
        pl.semaphore_signal(barrier, inc=1, device_id=on_tp((tp + j) % 8), device_id_type=MESH)
    for dy in range(NY):
        for dz in range(NZ):
            if dy or dz:
                other = ((y + dy) % NY) * NZ + (z + dz) % NZ
                pl.semaphore_signal(barrier, inc=1, device_id=on_ep(other), device_id_type=MESH)
    small[0].wait()
    small[1].wait()
    info_ref[0:2, :] = jnp.concatenate([routes_ref[...].astype(F32)] * 8, axis=1)
    info_ref[2:4, :] = jnp.concatenate([combine_ref[...]] * 8, axis=1)
    info_ref[4:8, :] = jnp.zeros((4, 128), F32)
    small[2].wait()
    pl.semaphore_wait(barrier, 22)

    def ring_cols(h, t):
        return pl.ds(pl.multiple_of(t * RING[h], 128), RING[h])

    def direct_cols(h, core):
        return pl.ds(pl.multiple_of(8 * RING[h] + core * DIRECT[h], 128), DIRECT[h])

    peers = [(tp + j) % 8 for j in (4, 5, 3, 2, 6, 7, 1)]
    for t in peers:
        remote(0, "info", info_ref, infos.at[tp], on_tp(t))
    for h in (A, B):
        for t in peers:
            remote(0, ("t2", h), tok_ref.at[:, ring_cols(h, t)], half[h].t2.at[tp], on_tp(t))
    for t in peers:
        remote(0, ("t1", A), tok_ref.at[:, direct_cols(A, t % 2)], half[A].t1.at[tp], on_tp(t))
    infos[tp] = info_ref[...]
    for h in (A, B):
        half[h].t2[tp] = tok_ref[:, ring_cols(h, tp)]
        half[h].t1[tp] = tok_ref[:, direct_cols(h, c)]
    loads = []
    for n, (src, dst) in enumerate(((wg_hbm, wg), (wu_hbm, wu), (wd_hbm, wd))):
        load = pltpu.make_async_copy(src, dst, w_sem.at[n])
        load.start()
        loads.append(load)
    row = lax.broadcasted_iota(jnp.int32, (512, 128), 0)
    lane = lax.broadcasted_iota(jnp.int32, (512, 128), 1)
    j_of = (row // 32) % 8
    dy_of = j_of // 2
    dz_of = (2 * (j_of % 2) + dy_of + row // 256) % NZ
    expert_of[...] = (((y + dy_of) % NY) * NZ + (z + dz_of) % NZ).astype(F32)
    same = (lane // 16) == ((row % 32) // 4)
    slot_of[...] = jnp.where(same, row % 4, 128).astype(F32)
    urow = lax.broadcasted_iota(jnp.int32, (128, 128), 0)
    ulane = lax.broadcasted_iota(jnp.int32, (128, 128), 1)
    total_ref[...] = jnp.zeros((16, 4096), F32)
    to = lax.broadcasted_iota(jnp.int32, (256, 256), 0)
    come = lax.broadcasted_iota(jnp.int32, (256, 256), 1)
    home = (x + to // 64) % NX
    perm[...] = jnp.where(come == ((to % 64) // 8) * 32 + home * 8 + to % 8, 1.0, 0.0).astype(BF16)
    before[...] = jnp.where((urow < ulane) & ((urow // 16) == (ulane // 16)), 1.0, 0.0).astype(BF16)
    arrived("info", infos.at[pl.ds(0, 7)])
    for t in peers:
        remote(0, ("t1", B), tok_ref.at[:, direct_cols(B, t % 2)], half[B].t1.at[tp], on_tp(t))

    lane8 = lax.broadcasted_iota(jnp.int32, (8, 128), 1) // 16
    info = jnp.zeros((8, 128), F32)
    for b in range(8):
        info = info + jnp.where(lane8 == b, infos[b], 0.0)
    expert = expert_of[...]
    first_of = jnp.where(info[0:1] == expert, 1.0, 0.0)
    second_of = jnp.where(info[1:2] == expert, 1.0, 0.0)
    named = first_of + second_of
    count = jnp.dot(named.astype(BF16), before[...], preferred_element_type=F32)
    hit = count == slot_of[...]
    sel[...] = jnp.where(hit, named, 0.0).astype(BF16)

    def pick(h, tokens, width, picked, landing, name):
        rows = sel[h * 256:(h + 1) * 256]
        got = jnp.dot(rows, tokens[...].reshape(128, width), preferred_element_type=F32)
        picked[...] = got.astype(BF16).reshape(8, 32, width)
        order = (4, 5, 6, 7, 2, 3, 1, 0) if h == A else (4, 5, 6, 2, 3, 7, 0, 1)
        for j in order:
            dy, dz = hop(h, j)
            if dy or dz:
                other = ((y + dy) % NY) * NZ + (z + dz) % NZ
                remote(0, (name, h), picked.at[j], landing.at[j], on_ep(other))
            else:
                landing[j] = picked[j]

    def others(h):
        return pl.ds(0, 7 if h == A else 8)

    def pick_ring(h):
        arrived(("t2", h), half[h].t2.at[pl.ds(0, 7)])
        pick(h, half[h].t2, RING[h], half[h].p2, half[h].x2.at[tp], "spread2")

    def pick_direct(h):
        arrived(("t1", h), half[h].t1.at[pl.ds(0, 7)])
        pick(h, half[h].t1, DIRECT[h], half[h].p1, half[h].x1.at[c], "spread1")

    pick_ring(A)
    pick_ring(B)
    weight = jnp.where(hit, first_of * info[2:3] + second_of * info[3:4], 0.0)
    wrows[...] = weight.reshape(16, 32, 128)
    weight = weight.T
    high = weight.astype(BF16)
    whi[...] = high
    wlo[...] = (weight - high.astype(F32)).astype(BF16)
    wcols[...] = wrows[:, pl.ds(pl.multiple_of(x * 8, 8), 8), :].reshape(128, 128).T
    mine = wcols[pl.ds(pl.multiple_of(x * 32, 32), 32), :]
    for h in (A, B):
        part = mine[:, h * 64:(h + 1) * 64]
        high = part.astype(BF16)
        half[h].w2hi[...] = high
        half[h].w2lo[...] = (part - high.astype(F32)).astype(BF16)

    LO, HI, ALL = pl.ds(0, 4), pl.ds(4, 4), pl.ds(0, 8)

    def push(name, t, h, rows, device):
        block = half[h].x2.at[t, rows]
        remote(1, (name, h), block, block, on_tp(device))

    def got(name, h, rows):
        arrived((name, h), half[h].x2.at[0, rows])

    def own_first(h):
        push("m_own", tp, h, ALL, mate)
        push("r_lo", tp, h, LO, right)
        push("l_hi", tp, h, HI, left)

    def own_second(h):
        push("r_hi", tp, h, HI, right)
        push("l_lo", tp, h, LO, left)

    def forward(h):
        got("r_lo", h, LO)
        push("m_left", left, h, LO, mate)
        push("f_lo", left, h, LO, right)
        got("l_hi", h, HI)
        push("m_right", right, h, HI, mate)
        push("f_hi", right, h, HI, left)

    def near_rest(h):
        got("r_hi", h, HI)
        push("m_left", left, h, HI, mate)
        got("l_lo", h, LO)
        push("m_right", right, h, LO, mate)

    def far_rest(h):
        got("f_lo", h, LO)
        push("m_far", far, h, LO, mate)
        got("f_hi", h, HI)
        push("m_far", far, h, HI, mate)

    def direct_share(h):
        x1 = half[h].x1
        arrived(("spread1", h), x1.at[0, others(h)])
        remote(1, ("m_direct", h), x1.at[c], x1.at[c], on_tp(mate))

    def accumulate(h, a, rows, fresh):
        gate = jnp.dot(a, wg[rows, :], preferred_element_type=F32)
        up = jnp.dot(a, wu[rows, :], preferred_element_type=F32)
        if fresh:
            half[h].accg[...] = gate
            half[h].accu[...] = up
        else:
            half[h].accg[...] += gate
            half[h].accu[...] += up

    def gate_up(h, k, name):
        got(name, h, ALL)
        chip = (x + k) % NX
        x2, r = half[h].x2, RING[h]
        a = jnp.concatenate([x2[chip * 2].reshape(256, r), x2[chip * 2 + 1].reshape(256, r)], axis=1)
        accumulate(h, a, pl.ds(pl.multiple_of(chip * 2 * r, 256), 2 * r), k == 0)

    def gate_up_part(h, k, core, name):
        if name is not None:
            got(name, h, ALL)
        t = ((x + k) % NX) * 2 + core
        r = RING[h]
        accumulate(h, half[h].x2[t].reshape(256, r), ring_cols(h, t), False)

    def gate_up_direct_own(h):
        accumulate(h, half[h].x1[c].reshape(256, DIRECT[h]), direct_cols(h, c), False)

    def gate_up_direct_mate(h):
        arrived(("m_direct", h), half[h].x1.at[0])
        accumulate(h, half[h].x1[1 - c].reshape(256, DIRECT[h]), direct_cols(h, 1 - c), False)

    def silu(h):
        gate = half[h].accg[...]
        half[h].hid[...] = (gate / (1.0 + jnp.exp(-gate)) * half[h].accu[...]).astype(BF16)
        half[h].hidp[...] = jnp.dot(perm[...], half[h].hid[...], preferred_element_type=F32).astype(BF16)

    def down(h, g):
        s, r = half[h], RING[h]
        parts = []
        for m in (2 * g, 2 * g + 1):
            cols = pl.ds(m * 2 * r, 2 * r)
            parts.append(jnp.dot(s.hidp[...], wd[:, cols], preferred_element_type=F32).astype(BF16))
        for m, part in zip((2 * g, 2 * g + 1), parts):
            for core in range(2):
                s.part2[core, :, m] = part[:, core * r:(core + 1) * r].reshape(4, 64, r)
        chunks = pl.ds(2 * g, 2)
        remote(2, ("far", h, g), s.part2.at[1 - c, 2, chunks], s.mate2.at[2, chunks], on_tp(mate))
        if g:
            for k in (1, 3, 0):
                remote(2, ("pair", h, k), s.part2.at[1 - c, k], s.mate2.at[k], on_tp(mate))

    def down_direct(h):
        s, d = half[h], DIRECT[h]
        for core in range(2):
            cols = pl.ds(8 * RING[h] + core * d, d)
            part = jnp.dot(s.hid[...], wd[:, cols], preferred_element_type=F32).astype(BF16)
            s.part1[core] = part.reshape(8, 32, d)
        remote(2, ("pair_direct", h), s.part1.at[1 - c], s.mate1, on_tp(mate))

    def paired(h, k):
        arrived(("pair", h, k), half[h].mate2.at[k])

    def chip_sum(h, k, rows, chunks=slice(None)):
        s = half[h]
        rows = pl.ds(rows * 32, 32)
        return s.part2[c, k, chunks, rows, :].astype(F32) + s.mate2[k, chunks, rows, :].astype(F32)

    def reduce_far(h, g):
        s = half[h]
        chunks = pl.ds(2 * g, 2)
        arrived(("far", h, g), s.mate2.at[2, chunks])
        for rows, name, device in ((0, "far_lo", right), (1, "far_hi", left)):
            s.far_s[rows, chunks] = chip_sum(h, 2, rows, chunks).astype(BF16)
            remote(2, (name, h, g), s.far_s.at[rows, chunks], s.far_r.at[rows, chunks], on_tp(device))

    def near_send(h, side, rows, value, chunks=pl.ds(0, 4)):
        s = half[h]
        s.near_s[side, rows, chunks] = value.astype(BF16)
        name = ("near_hi" if rows else "near_lo", h)
        at = (side, rows, chunks)
        remote(2, name, s.near_s.at[at], s.near_r.at[at], on_tp((right, left)[side]))

    def reduce_near_first(h):
        paired(h, 1)
        near_send(h, 0, 1, chip_sum(h, 1, 1))
        paired(h, 3)
        near_send(h, 1, 0, chip_sum(h, 3, 0))

    def reduce_near_second(h, g):
        s = half[h]
        chunks = pl.ds(2 * g, 2)
        arrived(("far_lo", h, g), s.far_r.at[0, chunks])
        near_send(h, 0, 0, chip_sum(h, 1, 0, chunks) + s.far_r[0, chunks].astype(F32), chunks)
        arrived(("far_hi", h, g), s.far_r.at[1, chunks])
        near_send(h, 1, 1, chip_sum(h, 3, 1, chunks) + s.far_r[1, chunks].astype(F32), chunks)

    def give_back(h, blocks, fin, landing, name):
        for j in blocks:
            at = (slice(None), j) if name == "back2" else (j,)
            dy, dz = hop(h, j)
            if dy or dz:
                other = ((y + NY - dy) % NY) * NZ + (z + NZ - dz) % NZ
                remote(3, (name, h), fin.at[at], landing.at[at], on_ep(other))
            else:
                landing[at] = fin[at]

    def reduce_last(h, parts):
        s = half[h]
        if 1 in parts:
            paired(h, 0)
        near_r = s.near_r
        for rows in parts:
            arrived(("near_hi" if rows else "near_lo", h), near_r.at[0])
            total = chip_sum(h, 0, rows)
            total = total + near_r[0, rows].astype(F32) + near_r[1, rows].astype(F32)
            s.fin2[:, rows * 4:rows * 4 + 4] = total.reshape(4, 4, 8, RING[h]).astype(BF16)
            give_back(h, range(rows * 4, rows * 4 + 4), s.fin2, s.r2, "back2")

    def direct_back(h):
        s = half[h]
        arrived(("pair_direct", h), s.mate1)
        s.fin1[...] = (s.part1[c].astype(F32) + s.mate1[...].astype(F32)).astype(BF16)
        give_back(h, (4, 5, 6, 7, 2, 3, 0, 1), s.fin1, s.r1, "back1")

    def weigh_ring(h):
        s, r = half[h], RING[h]
        arrived(("back2", h), s.r2.at[:, others(h)])
        for m in range(NX):
            rows = s.r2[m].astype(F32).reshape(64, r).astype(BF16)
            total = jnp.dot(s.w2hi[...], rows, preferred_element_type=F32)
            total = total + jnp.dot(s.w2lo[...], rows, preferred_element_type=F32)
            s.o2s[:, m] = total.astype(BF16).reshape(2, 16, r)
        remote(3, ("out2", h), s.o2s.at[1 - c], s.o2r, on_tp(mate))

    def weigh_direct(h):
        s, d = half[h], DIRECT[h]
        arrived(("back1", h), s.r1.at[others(h)])
        rows = s.r1[...].reshape(256, d)
        cols = slice(h * 256, (h + 1) * 256)
        total = jnp.dot(whi[:, cols], rows, preferred_element_type=F32)
        total = total + jnp.dot(wlo[:, cols], rows, preferred_element_type=F32)
        s.o1s[...] = total.astype(BF16).reshape(8, 16, d)
        for t in peers:
            remote(3, ("out1", h), s.o1s.at[t], s.o1r.at[tp], on_tp(t))
        s.o1r[tp] = s.o1s[tp]

    def put(cols, value):
        total_ref[:, cols] += value

    def finish_direct(h):
        s, d = half[h], DIRECT[h]
        arrived(("out1", h), s.o1r.at[pl.ds(0, 7)])
        for core in range(2):
            piece = s.o1r[core].astype(F32)
            for chip in range(1, NX):
                piece = piece + s.o1r[chip * 2 + core].astype(F32)
            put(pl.ds(8 * RING[h] + core * d, d), piece)

    def finish_ring(h):
        s = half[h]
        arrived(("out2", h), s.o2r)
        for m in range(NX):
            put(ring_cols(h, 2 * m + c), s.o2s[c, m].astype(F32))
            put(ring_cols(h, 2 * m + 1 - c), s.o2r[m].astype(F32))

    pick_direct(A)
    arrived(("spread2", A), half[A].x2.at[0, others(A)])
    own_first(A)
    own_second(A)
    loads[0].wait()
    loads[1].wait()
    gate_up(A, 0, "m_own")
    arrived(("spread2", B), half[B].x2.at[0, others(B)])
    forward(A)
    own_first(B)
    own_second(B)
    pick_direct(B)
    near_rest(A)
    gate_up(A, 3, "m_left")
    gate_up(A, 1, "m_right")
    gate_up(B, 0, "m_own")
    far_rest(A)
    direct_share(A)
    gate_up_part(A, 2, c, None)
    gate_up_direct_own(A)
    gate_up_part(A, 2, 1 - c, "m_far")
    forward(B)
    gate_up_direct_mate(A)
    direct_share(B)
    silu(A)
    loads[2].wait()
    down(A, 0)
    down(A, 1)
    near_rest(B)
    down_direct(A)
    reduce_far(A, 0)
    reduce_far(A, 1)
    gate_up_direct_own(B)
    gate_up_direct_mate(B)
    far_rest(B)
    reduce_near_first(A)
    gate_up(B, 3, "m_left")
    gate_up(B, 1, "m_right")
    direct_back(A)
    gate_up_part(B, 2, c, None)
    gate_up_part(B, 2, 1 - c, "m_far")
    silu(B)
    down(B, 0)
    reduce_near_second(A, 0)
    reduce_near_second(A, 1)
    down(B, 1)
    reduce_far(B, 0)
    reduce_far(B, 1)
    reduce_near_first(B)
    down_direct(B)
    direct_back(B)
    reduce_last(A, (1, 0))
    reduce_near_second(B, 0)
    reduce_near_second(B, 1)
    reduce_last(B, (1,))
    weigh_direct(A)
    reduce_last(B, (0,))
    weigh_direct(B)
    weigh_ring(A)
    weigh_ring(B)
    finish_ring(A)
    finish_ring(B)
    finish_direct(A)
    finish_direct(B)
    pass
    out_ref[...] = total_ref[...].astype(BF16)
    for group in range(4):
        every = tally.at[pl.ds(0, sent[group])]
        pltpu.make_async_remote_copy(
            src_ref=every, dst_ref=every, send_sem=send_sems.at[group], recv_sem=recv_sems.at[0],
            device_id=on_tp(mate), device_id_type=MESH,
        ).wait_send()
    assert len(recv_of) == RECVS, len(recv_of)


def body(tokens, routes, combine, gate_weight, up_weight, down_weight):
    vmem = pl.BlockSpec(memory_space=pltpu.VMEM)
    hbm = pl.BlockSpec(memory_space=pltpu.HBM)
    dma = pltpu.SemaphoreType.DMA
    return pl.pallas_call(
        kernel,
        out_shape=jax.ShapeDtypeStruct((16, 4096), BF16),
        in_specs=[hbm] * 6,
        out_specs=vmem,
        scratch_shapes=[
            pltpu.VMEM((16, 4096), BF16),
            pltpu.VMEM((2, 16), jnp.int32),
            pltpu.VMEM((2, 16), F32),
            pltpu.VMEM((8, 128), F32),
            pltpu.VMEM((8, 8, 128), F32),
            pltpu.VMEM((4096, 512), BF16),
            pltpu.VMEM((4096, 512), BF16),
            pltpu.VMEM((512, 4096), BF16),
            pltpu.VMEM((512, 128), BF16),
            pltpu.VMEM((128, 512), BF16),
            pltpu.VMEM((128, 512), BF16),
            pltpu.VMEM((TALLY, 8, 128), F32),
            pltpu.VMEM((512, 128), F32),
            pltpu.VMEM((512, 128), F32),
            pltpu.VMEM((128, 128), BF16),
            pltpu.VMEM((256, 256), BF16),
            pltpu.VMEM((16, 32, 128), F32),
            pltpu.VMEM((128, 128), F32),
            pltpu.VMEM((16, 4096), F32),
            dma((6,)),
            dma((4,)),
            dma((RECVS,)),
            *half_scratch(A),
            *half_scratch(B),
        ],
        compiler_params=pltpu.CompilerParams(
            collective_id=0, has_side_effects=True, vmem_limit_bytes=60 * 1024 * 1024
        ),
        name="moe",
    )(tokens, routes.T, combine.T, gate_weight[0], up_weight[0], down_weight[0])


def solution(mesh):
    return jax.shard_map(
        body,
        mesh=mesh,
        in_specs=(
            P(("ep", "tp"), None),
            P(("ep", "tp"), None),
            P(("ep", "tp"), None),
            P("ep", None, "tp"),
            P("ep", None, "tp"),
            P("ep", "tp", None),
        ),
        out_specs=P(("ep", "tp"), None),
        check_vma=False,
    )
```

```python
from typing import Any, NamedTuple

import jax
import jax.numpy as jnp
from jax import lax
from jax.experimental import pallas as pl
from jax.experimental.pallas import tpu as pltpu
from jax.sharding import PartitionSpec as P

MESH = pl.DeviceIdType.MESH
F32 = jnp.float32
BF16 = jnp.bfloat16
NX, NY, NZ = 4, 4, 4
A, B = 0, 1
RING = (256, 384)
DIRECT = (1024, 512)
RECVS = 63
TALLY = 1024


def hop(h, j):
    dy = j // 2
    return dy, (2 * (j % 2) + dy + h) % NZ


class Half(NamedTuple):
    t2: Any
    t1: Any
    p2: Any
    p1: Any
    x2: Any
    x1: Any
    accg: Any
    accu: Any
    hid: Any
    hidp: Any
    part2: Any
    mate2: Any
    part1: Any
    mate1: Any
    far_s: Any
    far_r: Any
    near_s: Any
    near_r: Any
    fin2: Any
    fin1: Any
    r2: Any
    r1: Any
    o2s: Any
    o1s: Any
    o2r: Any
    o1r: Any
    w2hi: Any
    w2lo: Any


def half_scratch(h):
    r, d = RING[h], DIRECT[h]
    bf = lambda *shape: pltpu.VMEM(shape, BF16)
    f = lambda *shape: pltpu.VMEM(shape, F32)
    return Half(
        t2=bf(8, 16, r), t1=bf(8, 16, d), p2=bf(8, 32, r), p1=bf(8, 32, d),
        x2=bf(8, 8, 32, r), x1=bf(2, 8, 32, d),
        accg=f(256, 512), accu=f(256, 512), hid=bf(256, 512), hidp=bf(256, 512),
        part2=bf(2, 4, 4, 64, r), mate2=bf(4, 4, 64, r), part1=bf(2, 8, 32, d), mate1=bf(8, 32, d),
        far_s=bf(2, 4, 32, r), far_r=bf(2, 4, 32, r), near_s=bf(2, 2, 4, 32, r), near_r=bf(2, 2, 4, 32, r),
        fin2=bf(4, 8, 8, r), fin1=bf(8, 32, d), r2=bf(4, 8, 8, r), r1=bf(8, 32, d),
        o2s=bf(2, 4, 16, r), o1s=bf(8, 16, d), o2r=bf(4, 16, r), o1r=bf(8, 16, d),
        w2hi=bf(32, 64), w2lo=bf(32, 64),
    )


def kernel(
    tok_hbm, routes_hbm, combine_hbm, wg_hbm, wu_hbm, wd_hbm, out_ref,
    tok_ref, routes_ref, combine_ref, info_ref, infos, wg, wu, wd, sel, whi, wlo, tally, expert_of, slot_of, before, perm, wrows, wcols, total_ref,
    w_sem, send_sems, recv_sems, *halves,
):
    half = [Half(*halves[:len(Half._fields)]), Half(*halves[len(Half._fields):])]
    ep = lax.axis_index("ep")
    tp = lax.axis_index("tp")
    y, z = ep // NZ, ep % NZ
    x, c = tp // 2, tp % 2
    recv_of = {}
    sent = [0, 0, 0, 0]

    def on_tp(other):
        return {"ep": ep, "tp": other}

    def on_ep(other):
        return {"ep": other, "tp": tp}

    def recv_sem(name):
        return recv_sems.at[recv_of.setdefault(name, len(recv_of))]

    def remote(group, name, src, dst, device):
        size = src.dtype.itemsize
        for dim in src.shape:
            size *= dim
        sent[group] += size // 4096
        pltpu.make_async_remote_copy(
            src_ref=src, dst_ref=dst, send_sem=send_sems.at[group], recv_sem=recv_sem(name),
            device_id=device, device_id_type=MESH,
        ).start()

    def arrived(name, like):
        pltpu.make_async_remote_copy(
            src_ref=like, dst_ref=like, send_sem=send_sems.at[0], recv_sem=recv_sem(name),
            device_id=on_tp(mate), device_id_type=MESH,
        ).wait_recv()

    mate = x * 2 + (1 - c)
    right = ((x + 1) % NX) * 2 + c
    left = ((x + 3) % NX) * 2 + c
    far = ((x + 2) % NX) * 2 + c

    small = []
    for n, (src, dst) in enumerate(
        ((routes_hbm, routes_ref), (combine_hbm, combine_ref), (tok_hbm, tok_ref))
    ):
        load = pltpu.make_async_copy(src, dst, w_sem.at[3 + n])
        load.start()
        small.append(load)
    barrier = pltpu.get_barrier_semaphore()
    for j in range(1, 8):
        pl.semaphore_signal(barrier, inc=1, device_id=on_tp((tp + j) % 8), device_id_type=MESH)
    for dy in range(NY):
        for dz in range(NZ):
            if dy or dz:
                other = ((y + dy) % NY) * NZ + (z + dz) % NZ
                pl.semaphore_signal(barrier, inc=1, device_id=on_ep(other), device_id_type=MESH)
    small[0].wait()
    small[1].wait()
    info_ref[0:2, :] = jnp.concatenate([routes_ref[...].astype(F32)] * 8, axis=1)
    info_ref[2:4, :] = jnp.concatenate([combine_ref[...]] * 8, axis=1)
    info_ref[4:8, :] = jnp.zeros((4, 128), F32)
    small[2].wait()
    pl.semaphore_wait(barrier, 22)

    def ring_cols(h, t):
        return pl.ds(pl.multiple_of(t * RING[h], 128), RING[h])

    def direct_cols(h, core):
        return pl.ds(pl.multiple_of(8 * RING[h] + core * DIRECT[h], 128), DIRECT[h])

    peers = [(tp + j) % 8 for j in (4, 5, 3, 2, 6, 7, 1)]
    for t in peers:
        remote(0, "info", info_ref, infos.at[tp], on_tp(t))
    for h in (A, B):
        for t in peers:
            remote(0, ("t2", h), tok_ref.at[:, ring_cols(h, t)], half[h].t2.at[tp], on_tp(t))
    for t in peers:
        remote(0, ("t1", A), tok_ref.at[:, direct_cols(A, t % 2)], half[A].t1.at[tp], on_tp(t))
    infos[tp] = info_ref[...]
    for h in (A, B):
        half[h].t2[tp] = tok_ref[:, ring_cols(h, tp)]
        half[h].t1[tp] = tok_ref[:, direct_cols(h, c)]
    loads = []
    for n, (src, dst) in enumerate(((wg_hbm, wg), (wu_hbm, wu), (wd_hbm, wd))):
        load = pltpu.make_async_copy(src, dst, w_sem.at[n])
        load.start()
        loads.append(load)
    row = lax.broadcasted_iota(jnp.int32, (512, 128), 0)
    lane = lax.broadcasted_iota(jnp.int32, (512, 128), 1)
    j_of = (row // 32) % 8
    dy_of = j_of // 2
    dz_of = (2 * (j_of % 2) + dy_of + row // 256) % NZ
    expert_of[...] = (((y + dy_of) % NY) * NZ + (z + dz_of) % NZ).astype(F32)
    same = (lane // 16) == ((row % 32) // 4)
    slot_of[...] = jnp.where(same, row % 4, 128).astype(F32)
    urow = lax.broadcasted_iota(jnp.int32, (128, 128), 0)
    ulane = lax.broadcasted_iota(jnp.int32, (128, 128), 1)
    total_ref[...] = jnp.zeros((16, 4096), F32)
    to = lax.broadcasted_iota(jnp.int32, (256, 256), 0)
    come = lax.broadcasted_iota(jnp.int32, (256, 256), 1)
    home = (x + to // 64) % NX
    perm[...] = jnp.where(come == ((to % 64) // 8) * 32 + home * 8 + to % 8, 1.0, 0.0).astype(BF16)
    before[...] = jnp.where((urow < ulane) & ((urow // 16) == (ulane // 16)), 1.0, 0.0).astype(BF16)
    arrived("info", infos.at[pl.ds(0, 7)])
    for t in peers:
        remote(0, ("t1", B), tok_ref.at[:, direct_cols(B, t % 2)], half[B].t1.at[tp], on_tp(t))

    lane8 = lax.broadcasted_iota(jnp.int32, (8, 128), 1) // 16
    info = jnp.zeros((8, 128), F32)
    for b in range(8):
        info = info + jnp.where(lane8 == b, infos[b], 0.0)
    expert = expert_of[...]
    first_of = jnp.where(info[0:1] == expert, 1.0, 0.0)
    second_of = jnp.where(info[1:2] == expert, 1.0, 0.0)
    named = first_of + second_of
    count = jnp.dot(named.astype(BF16), before[...], preferred_element_type=F32)
    hit = count == slot_of[...]
    sel[...] = jnp.where(hit, named, 0.0).astype(BF16)

    def pick(h, tokens, width, picked, landing, name):
        rows = sel[h * 256:(h + 1) * 256]
        got = jnp.dot(rows, tokens[...].reshape(128, width), preferred_element_type=F32)
        picked[...] = got.astype(BF16).reshape(8, 32, width)
        order = (4, 5, 6, 7, 2, 3, 1, 0) if h == A else (4, 5, 6, 2, 3, 7, 0, 1)
        for j in order:
            dy, dz = hop(h, j)
            if dy or dz:
                other = ((y + dy) % NY) * NZ + (z + dz) % NZ
                remote(0, (name, h), picked.at[j], landing.at[j], on_ep(other))
            else:
                landing[j] = picked[j]

    def others(h):
        return pl.ds(0, 7 if h == A else 8)

    def pick_ring(h):
        arrived(("t2", h), half[h].t2.at[pl.ds(0, 7)])
        pick(h, half[h].t2, RING[h], half[h].p2, half[h].x2.at[tp], "spread2")

    def pick_direct(h):
        arrived(("t1", h), half[h].t1.at[pl.ds(0, 7)])
        pick(h, half[h].t1, DIRECT[h], half[h].p1, half[h].x1.at[c], "spread1")

    pick_ring(A)
    pick_ring(B)
    weight = jnp.where(hit, first_of * info[2:3] + second_of * info[3:4], 0.0)
    wrows[...] = weight.reshape(16, 32, 128)
    weight = weight.T
    high = weight.astype(BF16)
    whi[...] = high
    wlo[...] = (weight - high.astype(F32)).astype(BF16)
    wcols[...] = wrows[:, pl.ds(pl.multiple_of(x * 8, 8), 8), :].reshape(128, 128).T
    mine = wcols[pl.ds(pl.multiple_of(x * 32, 32), 32), :]
    for h in (A, B):
        part = mine[:, h * 64:(h + 1) * 64]
        high = part.astype(BF16)
        half[h].w2hi[...] = high
        half[h].w2lo[...] = (part - high.astype(F32)).astype(BF16)

    LO, HI, ALL = pl.ds(0, 4), pl.ds(4, 4), pl.ds(0, 8)

    def push(name, t, h, rows, device):
        block = half[h].x2.at[t, rows]
        remote(1, (name, h), block, block, on_tp(device))

    def got(name, h, rows):
        arrived((name, h), half[h].x2.at[0, rows])

    def own_first(h):
        push("m_own", tp, h, ALL, mate)
        push("r_lo", tp, h, LO, right)
        push("l_hi", tp, h, HI, left)

    def own_second(h):
        push("r_hi", tp, h, HI, right)
        push("l_lo", tp, h, LO, left)

    def forward(h):
        got("r_lo", h, LO)
        push("m_left", left, h, LO, mate)
        push("f_lo", left, h, LO, right)
        got("l_hi", h, HI)
        push("m_right", right, h, HI, mate)
        push("f_hi", right, h, HI, left)

    def near_rest(h):
        got("r_hi", h, HI)
        push("m_left", left, h, HI, mate)
        got("l_lo", h, LO)
        push("m_right", right, h, LO, mate)

    def far_rest(h):
        got("f_lo", h, LO)
        push("m_far", far, h, LO, mate)
        got("f_hi", h, HI)
        push("m_far", far, h, HI, mate)

    def direct_share(h):
        x1 = half[h].x1
        arrived(("spread1", h), x1.at[0, others(h)])
        remote(1, ("m_direct", h), x1.at[c], x1.at[c], on_tp(mate))

    def accumulate(h, a, rows, fresh):
        gate = jnp.dot(a, wg[rows, :], preferred_element_type=F32)
        up = jnp.dot(a, wu[rows, :], preferred_element_type=F32)
        if fresh:
            half[h].accg[...] = gate
            half[h].accu[...] = up
        else:
            half[h].accg[...] += gate
            half[h].accu[...] += up

    def gate_up(h, k, name):
        got(name, h, ALL)
        chip = (x + k) % NX
        x2, r = half[h].x2, RING[h]
        a = jnp.concatenate([x2[chip * 2].reshape(256, r), x2[chip * 2 + 1].reshape(256, r)], axis=1)
        accumulate(h, a, pl.ds(pl.multiple_of(chip * 2 * r, 256), 2 * r), k == 0)

    def gate_up_part(h, k, core, name):
        if name is not None:
            got(name, h, ALL)
        t = ((x + k) % NX) * 2 + core
        r = RING[h]
        accumulate(h, half[h].x2[t].reshape(256, r), ring_cols(h, t), False)

    def gate_up_direct_own(h):
        accumulate(h, half[h].x1[c].reshape(256, DIRECT[h]), direct_cols(h, c), False)

    def gate_up_direct_mate(h):
        arrived(("m_direct", h), half[h].x1.at[0])
        accumulate(h, half[h].x1[1 - c].reshape(256, DIRECT[h]), direct_cols(h, 1 - c), False)

    def silu(h):
        gate = half[h].accg[...]
        half[h].hid[...] = (gate / (1.0 + jnp.exp(-gate)) * half[h].accu[...]).astype(BF16)
        half[h].hidp[...] = jnp.dot(perm[...], half[h].hid[...], preferred_element_type=F32).astype(BF16)

    def down(h, g):
        s, r = half[h], RING[h]
        parts = []
        for m in (2 * g, 2 * g + 1):
            cols = pl.ds(m * 2 * r, 2 * r)
            parts.append(jnp.dot(s.hidp[...], wd[:, cols], preferred_element_type=F32).astype(BF16))
        for m, part in zip((2 * g, 2 * g + 1), parts):
            for core in range(2):
                s.part2[core, :, m] = part[:, core * r:(core + 1) * r].reshape(4, 64, r)
        chunks = pl.ds(2 * g, 2)
        remote(2, ("far", h, g), s.part2.at[1 - c, 2, chunks], s.mate2.at[2, chunks], on_tp(mate))
        if g:
            for k in (1, 3, 0):
                remote(2, ("pair", h, k), s.part2.at[1 - c, k], s.mate2.at[k], on_tp(mate))

    def down_direct(h):
        s, d = half[h], DIRECT[h]
        for core in range(2):
            cols = pl.ds(8 * RING[h] + core * d, d)
            part = jnp.dot(s.hid[...], wd[:, cols], preferred_element_type=F32).astype(BF16)
            s.part1[core] = part.reshape(8, 32, d)
        remote(2, ("pair_direct", h), s.part1.at[1 - c], s.mate1, on_tp(mate))

    def paired(h, k):
        arrived(("pair", h, k), half[h].mate2.at[k])

    def chip_sum(h, k, rows, chunks=slice(None)):
        s = half[h]
        rows = pl.ds(rows * 32, 32)
        return s.part2[c, k, chunks, rows, :].astype(F32) + s.mate2[k, chunks, rows, :].astype(F32)

    def reduce_far(h, g):
        s = half[h]
        chunks = pl.ds(2 * g, 2)
        arrived(("far", h, g), s.mate2.at[2, chunks])
        for rows, name, device in ((0, "far_lo", right), (1, "far_hi", left)):
            s.far_s[rows, chunks] = chip_sum(h, 2, rows, chunks).astype(BF16)
            remote(2, (name, h, g), s.far_s.at[rows, chunks], s.far_r.at[rows, chunks], on_tp(device))

    def near_send(h, side, rows, value, chunks=pl.ds(0, 4)):
        s = half[h]
        s.near_s[side, rows, chunks] = value.astype(BF16)
        name = ("near_hi" if rows else "near_lo", h)
        at = (side, rows, chunks)
        remote(2, name, s.near_s.at[at], s.near_r.at[at], on_tp((right, left)[side]))

    def reduce_near_first(h):
        paired(h, 1)
        near_send(h, 0, 1, chip_sum(h, 1, 1))
        paired(h, 3)
        near_send(h, 1, 0, chip_sum(h, 3, 0))

    def reduce_near_second(h, g):
        s = half[h]
        chunks = pl.ds(2 * g, 2)
        arrived(("far_lo", h, g), s.far_r.at[0, chunks])
        near_send(h, 0, 0, chip_sum(h, 1, 0, chunks) + s.far_r[0, chunks].astype(F32), chunks)
        arrived(("far_hi", h, g), s.far_r.at[1, chunks])
        near_send(h, 1, 1, chip_sum(h, 3, 1, chunks) + s.far_r[1, chunks].astype(F32), chunks)

    def give_back(h, blocks, fin, landing, name):
        for j in blocks:
            at = (slice(None), j) if name == "back2" else (j,)
            dy, dz = hop(h, j)
            if dy or dz:
                other = ((y + NY - dy) % NY) * NZ + (z + NZ - dz) % NZ
                remote(3, (name, h), fin.at[at], landing.at[at], on_ep(other))
            else:
                landing[at] = fin[at]

    def reduce_last(h):
        s = half[h]
        paired(h, 0)
        near_r = s.near_r
        for rows, name in ((1, "near_hi"), (0, "near_lo")):
            arrived((name, h), near_r.at[0])
            total = chip_sum(h, 0, rows)
            total = total + near_r[0, rows].astype(F32) + near_r[1, rows].astype(F32)
            s.fin2[:, rows * 4:rows * 4 + 4] = total.reshape(4, 4, 8, RING[h]).astype(BF16)
            give_back(h, range(rows * 4, rows * 4 + 4), s.fin2, s.r2, "back2")

    def direct_back(h):
        s = half[h]
        arrived(("pair_direct", h), s.mate1)
        s.fin1[...] = (s.part1[c].astype(F32) + s.mate1[...].astype(F32)).astype(BF16)
        give_back(h, (4, 5, 6, 7, 2, 3, 0, 1), s.fin1, s.r1, "back1")

    def weigh_ring(h):
        s, r = half[h], RING[h]
        arrived(("back2", h), s.r2.at[:, others(h)])
        for m in range(NX):
            rows = s.r2[m].astype(F32).reshape(64, r).astype(BF16)
            total = jnp.dot(s.w2hi[...], rows, preferred_element_type=F32)
            total = total + jnp.dot(s.w2lo[...], rows, preferred_element_type=F32)
            s.o2s[:, m] = total.astype(BF16).reshape(2, 16, r)
        remote(3, ("out2", h), s.o2s.at[1 - c], s.o2r, on_tp(mate))

    def weigh_direct(h):
        s, d = half[h], DIRECT[h]
        arrived(("back1", h), s.r1.at[others(h)])
        cols = slice(h * 256, (h + 1) * 256)
        for start in range(0, d, 512):
            wide = pl.ds(start, 512)
            rows = s.r1[:, :, wide].reshape(256, 512)
            total = jnp.dot(whi[:, cols], rows, preferred_element_type=F32)
            total = total + jnp.dot(wlo[:, cols], rows, preferred_element_type=F32)
            s.o1s[:, :, wide] = total.astype(BF16).reshape(8, 16, 512)
            for t in peers:
                remote(3, ("out1", h), s.o1s.at[t, :, wide], s.o1r.at[tp, :, wide], on_tp(t))
        s.o1r[tp] = s.o1s[tp]

    def put(cols, value):
        total_ref[:, cols] += value

    def finish_direct(h):
        s, d = half[h], DIRECT[h]
        arrived(("out1", h), s.o1r.at[pl.ds(0, 7)])
        for core in range(2):
            piece = s.o1r[core].astype(F32)
            for chip in range(1, NX):
                piece = piece + s.o1r[chip * 2 + core].astype(F32)
            put(pl.ds(8 * RING[h] + core * d, d), piece)

    def finish_ring(h):
        s = half[h]
        arrived(("out2", h), s.o2r)
        for m in range(NX):
            put(ring_cols(h, 2 * m + c), s.o2s[c, m].astype(F32))
            put(ring_cols(h, 2 * m + 1 - c), s.o2r[m].astype(F32))

    pick_direct(A)
    arrived(("spread2", A), half[A].x2.at[0, others(A)])
    own_first(A)
    own_second(A)
    loads[0].wait()
    loads[1].wait()
    gate_up(A, 0, "m_own")
    arrived(("spread2", B), half[B].x2.at[0, others(B)])
    forward(A)
    own_first(B)
    own_second(B)
    pick_direct(B)
    near_rest(A)
    gate_up(A, 3, "m_left")
    gate_up(A, 1, "m_right")
    gate_up(B, 0, "m_own")
    far_rest(A)
    direct_share(A)
    gate_up_part(A, 2, c, None)
    gate_up_direct_own(A)
    gate_up_part(A, 2, 1 - c, "m_far")
    forward(B)
    gate_up_direct_mate(A)
    direct_share(B)
    silu(A)
    loads[2].wait()
    down(A, 0)
    down(A, 1)
    near_rest(B)
    down_direct(A)
    reduce_far(A, 0)
    reduce_far(A, 1)
    gate_up_direct_own(B)
    gate_up_direct_mate(B)
    far_rest(B)
    reduce_near_first(A)
    gate_up(B, 3, "m_left")
    gate_up(B, 1, "m_right")
    direct_back(A)
    gate_up_part(B, 2, c, None)
    gate_up_part(B, 2, 1 - c, "m_far")
    silu(B)
    down(B, 0)
    reduce_near_second(A, 0)
    reduce_near_second(A, 1)
    down(B, 1)
    reduce_far(B, 0)
    reduce_far(B, 1)
    reduce_near_first(B)
    down_direct(B)
    direct_back(B)
    reduce_last(A)
    reduce_near_second(B, 0)
    reduce_near_second(B, 1)
    reduce_last(B)
    weigh_direct(A)
    weigh_direct(B)
    weigh_ring(A)
    weigh_ring(B)
    finish_ring(A)
    finish_ring(B)
    finish_direct(A)
    finish_direct(B)
    pass
    out_ref[...] = total_ref[...].astype(BF16)
    for group in range(4):
        every = tally.at[pl.ds(0, sent[group])]
        pltpu.make_async_remote_copy(
            src_ref=every, dst_ref=every, send_sem=send_sems.at[group], recv_sem=recv_sems.at[0],
            device_id=on_tp(mate), device_id_type=MESH,
        ).wait_send()
    assert len(recv_of) == RECVS, len(recv_of)


def body(tokens, routes, combine, gate_weight, up_weight, down_weight):
    vmem = pl.BlockSpec(memory_space=pltpu.VMEM)
    hbm = pl.BlockSpec(memory_space=pltpu.HBM)
    dma = pltpu.SemaphoreType.DMA
    return pl.pallas_call(
        kernel,
        out_shape=jax.ShapeDtypeStruct((16, 4096), BF16),
        in_specs=[hbm] * 6,
        out_specs=vmem,
        scratch_shapes=[
            pltpu.VMEM((16, 4096), BF16),
            pltpu.VMEM((2, 16), jnp.int32),
            pltpu.VMEM((2, 16), F32),
            pltpu.VMEM((8, 128), F32),
            pltpu.VMEM((8, 8, 128), F32),
            pltpu.VMEM((4096, 512), BF16),
            pltpu.VMEM((4096, 512), BF16),
            pltpu.VMEM((512, 4096), BF16),
            pltpu.VMEM((512, 128), BF16),
            pltpu.VMEM((128, 512), BF16),
            pltpu.VMEM((128, 512), BF16),
            pltpu.VMEM((TALLY, 8, 128), F32),
            pltpu.VMEM((512, 128), F32),
            pltpu.VMEM((512, 128), F32),
            pltpu.VMEM((128, 128), BF16),
            pltpu.VMEM((256, 256), BF16),
            pltpu.VMEM((16, 32, 128), F32),
            pltpu.VMEM((128, 128), F32),
            pltpu.VMEM((16, 4096), F32),
            dma((6,)),
            dma((4,)),
            dma((RECVS,)),
            *half_scratch(A),
            *half_scratch(B),
        ],
        compiler_params=pltpu.CompilerParams(
            collective_id=0, has_side_effects=True, vmem_limit_bytes=60 * 1024 * 1024
        ),
        name="moe",
    )(tokens, routes.T, combine.T, gate_weight[0], up_weight[0], down_weight[0])


def solution(mesh):
    return jax.shard_map(
        body,
        mesh=mesh,
        in_specs=(
            P(("ep", "tp"), None),
            P(("ep", "tp"), None),
            P(("ep", "tp"), None),
            P("ep", None, "tp"),
            P("ep", None, "tp"),
            P("ep", "tp", None),
        ),
        out_specs=P(("ep", "tp"), None),
        check_vma=False,
    )
```
